32 devices in a mesh: dp: 16 (over z, y, core), seq: 2 (over x).
Axes of the slice: x: 2, y: 2, z: 4, core: 2. Of those that a mesh axis runs over, the one named last changes fastest.
Arguments:
- hidden: bfloat16 [16, 1024, 1536], P('dp', 'seq'), may hold values from -6 to 6
- cotangent: bfloat16 [16, 1024, 1536], P('dp', 'seq'), may hold values from -6 to 6
- segments: int32 [16, 1024], P('dp'), may hold values from 0 to 2, never falling along the last dimension, each value on 1 to 512 neighbouring positions
- weight_in: float32 [1536, 6448], P(('dp', 'seq')), may hold values from -0.15625 to 0.15625
- weight_out: float32 [3072, 1536], P(('dp', 'seq')), may hold values from -0.109375 to 0.109375
- gain_pre: float32 [1536], P(('dp', 'seq')), may hold values from 0.5 to 1.5
- gain_gated: float32 [3072], P(('dp', 'seq')), may hold values from 0.5 to 1.5
- conv_taps: float32 [4, 3328], P(None, ('dp', 'seq')), may hold values from -3 to 3
- conv_bias: float32 [3328], P(('dp', 'seq')), may hold values from -0.5 to 0.5
- decay_log: float32 [48], replicated, may hold values from 0 to 2.77
- skip_gain: float32 [48], replicated, may hold values from 0.5 to 1.5
- step_bias: float32 [48], replicated, may hold values from -7 to -2.3
- mean_weight_in: float32 [1536, 6448], P(('dp', 'seq')), may hold values from -16 to 16
- square_weight_in: float32 [1536, 6448], P(('dp', 'seq')), may hold values from 0.1 to 30
- mean_weight_out: float32 [3072, 1536], P(('dp', 'seq')), may hold values from -16 to 16
- square_weight_out: float32 [3072, 1536], P(('dp', 'seq')), may hold values from 0.1 to 30
- mean_gain_pre: float32 [1536], P(('dp', 'seq')), may hold values from -16 to 16
- square_gain_pre: float32 [1536], P(('dp', 'seq')), may hold values from 0.1 to 30
- mean_gain_gated: float32 [3072], P(('dp', 'seq')), may hold values from -16 to 16
- square_gain_gated: float32 [3072], P(('dp', 'seq')), may hold values from 0.1 to 30
- mean_conv_taps: float32 [4, 3328], P(None, ('dp', 'seq')), may hold values from -16 to 16
- square_conv_taps: float32 [4, 3328], P(None, ('dp', 'seq')), may hold values from 0.1 to 30
- mean_conv_bias: float32 [3328], P(('dp', 'seq')), may hold values from -16 to 16
- square_conv_bias: float32 [3328], P(('dp', 'seq')), may hold values from 0.1 to 30
- mean_decay_log: float32 [48], replicated, may hold values from -16 to 16
- square_decay_log: float32 [48], replicated, may hold values from 0.1 to 30
- mean_skip_gain: float32 [48], replicated, may hold values from -16 to 16
- square_skip_gain: float32 [48], replicated, may hold values from 0.1 to 30
- mean_step_bias: float32 [48], replicated, may hold values from -16 to 16
- square_step_bias: float32 [48], replicated, may hold values from 0.1 to 30
Outputs:
- output: bfloat16 [16, 1024, 1536], P('dp', 'seq')
- input_grad: float32 [16, 1024, 1536], P('dp', 'seq')
- grad_weight_in: float32 [1536, 6448], P(('dp', 'seq'))
- grad_weight_out: float32 [3072, 1536], P(('dp', 'seq'))
- grad_gain_pre: float32 [1536], P(('dp', 'seq'))
- grad_gain_gated: float32 [3072], P(('dp', 'seq'))
- grad_conv_taps: float32 [4, 3328], P(None, ('dp', 'seq'))
- grad_conv_bias: float32 [3328], P(('dp', 'seq'))
- grad_decay_log: float32 [48], replicated
- grad_skip_gain: float32 [48], replicated
- grad_step_bias: float32 [48], replicated
- new_weight_in: float32 [1536, 6448], P(('dp', 'seq'))
- new_weight_out: float32 [3072, 1536], P(('dp', 'seq'))
- new_gain_pre: float32 [1536], P(('dp', 'seq'))
- new_gain_gated: float32 [3072], P(('dp', 'seq'))
- new_conv_taps: float32 [4, 3328], P(None, ('dp', 'seq'))
- new_conv_bias: float32 [3328], P(('dp', 'seq'))
- new_decay_log: float32 [48], replicated
- new_skip_gain: float32 [48], replicated
- new_step_bias: float32 [48], replicated
- new_mean_weight_in: float32 [1536, 6448], P(('dp', 'seq'))
- new_mean_weight_out: float32 [3072, 1536], P(('dp', 'seq'))
- new_mean_gain_pre: float32 [1536], P(('dp', 'seq'))
- new_mean_gain_gated: float32 [3072], P(('dp', 'seq'))
- new_mean_conv_taps: float32 [4, 3328], P(None, ('dp', 'seq'))
- new_mean_conv_bias: float32 [3328], P(('dp', 'seq'))
- new_mean_decay_log: float32 [48], replicated
- new_mean_skip_gain: float32 [48], replicated
- new_mean_step_bias: float32 [48], replicated
- new_square_weight_in: float32 [1536, 6448], P(('dp', 'seq'))
- new_square_weight_out: float32 [3072, 1536], P(('dp', 'seq'))
- new_square_gain_pre: float32 [1536], P(('dp', 'seq'))
- new_square_gain_gated: float32 [3072], P(('dp', 'seq'))
- new_square_conv_taps: float32 [4, 3328], P(None, ('dp', 'seq'))
- new_square_conv_bias: float32 [3328], P(('dp', 'seq'))
- new_square_decay_log: float32 [48], replicated
- new_square_skip_gain: float32 [48], replicated
- new_square_step_bias: float32 [48], replicated
The draws below stay inside these ranges and needn't reach their ends.
Inputs may be any that keep to these rules, and one draw needn't show every extreme that they name: `segments`: in each sequence the segment numbers start at 0 and never fall, and all 3 documents are present, each of 1 to 512 tokens; some document holds exactly 512 tokens.
All inputs are finite; a program needn't handle non-finite values.
Results may differ from the reference program's by a relative error of at most 0.018.
The reference program's roundings to bfloat16 on the way count: a program that leaves them out, or rounds other values in their place, can miss the bound.
Values may be sent and summed in bfloat16 or wider, within the bound.
A program may use at most 384 MiB of HBM per device.

```python
import math
import jax
import jax.numpy as jnp
import numpy as np
from jax import lax

D = 1536
INNER = 3072
HEADS = 48
HEAD_DIM = 64
STATE = 128
CONV = 4
GROUP = 128
STEP = 4
LENGTH = 1024
SEQS = 16
XBC = 3328
PROJ = 6448


def strengthened(drawn, rng, source, target, blocks, factor):
    owner, partner = [(jnp.arange(drawn.shape[axis_at]) // (drawn.shape[axis_at] // blocks)).reshape([-1 if axis == axis_at else 1 for axis in range(drawn.ndim)]) for axis_at in (source, target)]
    chosen = jax.random.permutation(rng, blocks)[partner]
    strong = (owner == chosen) | (owner == (partner + blocks // 2) % blocks)
    return jnp.where(strong, factor * drawn, drawn)


def levels(key, extent, shards, smallest, largest):
    def one(position, parts):
        draws = jax.random.uniform(jax.random.fold_in(jax.random.fold_in(key, 6), position), (parts,), jnp.float32, smallest / len(shards), largest / len(shards))
        return jnp.repeat(jnp.exp(draws), extent[position] // parts).reshape((-1,) + (1,) * (len(extent) - position - 1))

    level = one(*shards[0])
    for cut in shards[1:]:
        level = level * one(*cut)
    return level


def profile(count, total, most, slope):
    weights = [(1 << 20) // math.isqrt(standing ** slope) + 1 for standing in range(2, count + 1)]
    spare, given = total - most - (count - 1), [1] * (count - 1)
    while spare > 0:
        candidates = [i for i in range(count - 1) if given[i] < most]
        whole, budget = sum([weights[i] for i in candidates]), spare
        for i in candidates:
            extra = min(most - given[i], max(1, budget * weights[i] // whole), spare)
            given[i] = given[i] + extra
            spare = spare - extra
    return np.array([most] + given)


def uneven(rng, amount, total, bound, skew):
    if amount == 2:
        one = jax.random.randint(rng, (), max(1, total - bound), min(bound, total - 1) + 1)
        return jnp.stack([one, total - one])
    lengths = jnp.asarray(profile(amount, total, bound, skew), jnp.int32)
    twos = (amount - 1) // 2
    donor, taker = lengths[1:1 + 2 * twos:2], lengths[2:2 + 2 * twos:2]
    slack = jnp.minimum(donor - 1, bound - taker)
    shifted = jax.random.randint(jax.random.fold_in(rng, 1), (twos,), 0, 1 << 20) % (slack + 1)
    lengths = lengths.at[1:1 + 2 * twos:2].set(donor - shifted).at[2:2 + 2 * twos:2].set(taker + shifted)
    return lengths[jax.random.permutation(jax.random.fold_in(rng, 2), amount)]


def bell_draw(own_key, dims, scale, most, shards=(), kind=jnp.bfloat16):
    level = levels(own_key, dims, shards, -0.22, 0.18) if shards else 1.0
    entries = jax.random.normal(own_key, dims, jnp.float32) * scale * level
    return jnp.minimum(jnp.maximum(entries, -most), most).astype(kind)


def bell_draw_with(own_key, dims, scale, bound, pieces, heavy, kind=jnp.bfloat16):
    drawn = scale * jax.random.normal(own_key, dims, jnp.float32)
    if pieces:
        drawn = drawn * levels(own_key, dims, pieces, -0.22, 0.18)
    return jnp.clip(strengthened(drawn, jax.random.fold_in(own_key, 3), *heavy), -bound, bound).astype(kind)


def setup_inputs(seed: int = 0) -> dict:
    streams_of = jax.random.split(jax.random.key(seed), 31)
    hidden = bell_draw_with(streams_of[0], (SEQS, LENGTH, D), 1.0, 6.0, ((0, 16), (1, 2)), (0, 2, 16, 2.0))
    cotangent = bell_draw(streams_of[1], (SEQS, LENGTH, D), 1.0, 6.0, ((0, 16), (1, 2)))
    segments = jax.vmap(lambda own: jnp.searchsorted(jnp.cumsum(uneven(own, 3, LENGTH, LENGTH // 2, 0)), jnp.arange(LENGTH), side="right"))(jax.random.split(streams_of[2], SEQS)).reshape((SEQS, LENGTH)).astype(jnp.int32)
    weight_in = bell_draw(streams_of[3], (D, PROJ), D ** -0.5, 0.15625, ((0, 32),), jnp.float32)
    weight_out = bell_draw(streams_of[4], (INNER, D), INNER ** -0.5, 0.109375, ((0, 32),), jnp.float32)
    gain_pre = jnp.clip(1.0 + 0.1 * jax.random.normal(streams_of[5], (D,), jnp.float32), 0.5, 1.5)
    gain_gated = jnp.clip(1.0 + 0.1 * jax.random.normal(streams_of[6], (INNER,), jnp.float32), 0.5, 1.5)
    conv_taps = bell_draw(streams_of[7], (CONV, XBC), CONV ** -0.5, 3.0, ((1, 32),), jnp.float32)
    conv_bias = jnp.clip(jax.random.uniform(streams_of[8], (XBC,), jnp.float32, -0.5, 0.5) * levels(streams_of[8], (XBC,), ((0, 32),), -0.4, 0.0), -0.5, 0.5)
    decay_log = jnp.clip(jax.random.uniform(streams_of[9], (HEADS,), jnp.float32, 0.0, 2.77), 0.0, 2.77)
    skip_gain = jnp.clip(jax.random.uniform(streams_of[10], (HEADS,), jnp.float32, 0.5, 1.5), 0.5, 1.5)
    step_bias = jnp.clip(jax.random.uniform(streams_of[11], (HEADS,), jnp.float32, -7.0, -2.3), -7.0, -2.3)
    mean_weight_in = bell_draw(streams_of[12], (D, PROJ), 3.0, 16.0, ((0, 32),), jnp.float32)
    square_weight_in = jnp.clip(jnp.exp(math.log(30.0) - 5.7037825 * jax.random.uniform(streams_of[13], (D, PROJ), jnp.float32) ** levels(streams_of[13], (D, PROJ), ((0, 32),), -0.2, 0.2)), 0.1, 30.0)
    mean_weight_out = bell_draw(streams_of[14], (INNER, D), 3.0, 16.0, ((0, 32),), jnp.float32)
    square_weight_out = jnp.clip(jnp.exp(math.log(30.0) - 5.7037825 * jax.random.uniform(streams_of[15], (INNER, D), jnp.float32) ** levels(streams_of[15], (INNER, D), ((0, 32),), -0.2, 0.2)), 0.1, 30.0)
    mean_gain_pre = bell_draw(streams_of[16], (D,), 3.0, 16.0, ((0, 32),), jnp.float32)
    square_gain_pre = jnp.clip(jnp.exp(math.log(30.0) - 5.7037825 * jax.random.uniform(streams_of[17], (D,), jnp.float32) ** levels(streams_of[17], (D,), ((0, 32),), -0.2, 0.2)), 0.1, 30.0)
    mean_gain_gated = bell_draw(streams_of[18], (INNER,), 3.0, 16.0, ((0, 32),), jnp.float32)
    square_gain_gated = jnp.clip(jnp.exp(math.log(30.0) - 5.7037825 * jax.random.uniform(streams_of[19], (INNER,), jnp.float32) ** levels(streams_of[19], (INNER,), ((0, 32),), -0.2, 0.2)), 0.1, 30.0)
    mean_conv_taps = bell_draw(streams_of[20], (CONV, XBC), 3.0, 16.0, ((1, 32),), jnp.float32)
    square_conv_taps = jnp.clip(jnp.exp(math.log(30.0) - 5.7037825 * jax.random.uniform(streams_of[21], (CONV, XBC), jnp.float32) ** levels(streams_of[21], (CONV, XBC), ((1, 32),), -0.2, 0.2)), 0.1, 30.0)
    mean_conv_bias = bell_draw(streams_of[22], (XBC,), 3.0, 16.0, ((0, 32),), jnp.float32)
    square_conv_bias = jnp.clip(jnp.exp(math.log(30.0) - 5.7037825 * jax.random.uniform(streams_of[23], (XBC,), jnp.float32) ** levels(streams_of[23], (XBC,), ((0, 32),), -0.2, 0.2)), 0.1, 30.0)
    mean_decay_log = bell_draw(streams_of[24], (HEADS,), 3.0, 16.0, (), jnp.float32)
    square_decay_log = jnp.clip(jnp.exp(jax.random.uniform(streams_of[25], (HEADS,), jnp.float32, math.log(0.1), math.log(30.0))), 0.1, 30.0)
    mean_skip_gain = bell_draw(streams_of[26], (HEADS,), 3.0, 16.0, (), jnp.float32)
    square_skip_gain = jnp.clip(jnp.exp(jax.random.uniform(streams_of[27], (HEADS,), jnp.float32, math.log(0.1), math.log(30.0))), 0.1, 30.0)
    mean_step_bias = bell_draw(streams_of[28], (HEADS,), 3.0, 16.0, (), jnp.float32)
    square_step_bias = jnp.clip(jnp.exp(jax.random.uniform(streams_of[29], (HEADS,), jnp.float32, math.log(0.1), math.log(30.0))), 0.1, 30.0)
    return {"hidden": hidden, "cotangent": cotangent, "segments": segments, "weight_in": weight_in, "weight_out": weight_out, "gain_pre": gain_pre, "gain_gated": gain_gated, "conv_taps": conv_taps, "conv_bias": conv_bias, "decay_log": decay_log, "skip_gain": skip_gain, "step_bias": step_bias, "mean_weight_in": mean_weight_in, "square_weight_in": square_weight_in, "mean_weight_out": mean_weight_out, "square_weight_out": square_weight_out, "mean_gain_pre": mean_gain_pre, "square_gain_pre": square_gain_pre, "mean_gain_gated": mean_gain_gated, "square_gain_gated": square_gain_gated, "mean_conv_taps": mean_conv_taps, "square_conv_taps": square_conv_taps, "mean_conv_bias": mean_conv_bias, "square_conv_bias": square_conv_bias, "mean_decay_log": mean_decay_log, "square_decay_log": square_decay_log, "mean_skip_gain": mean_skip_gain, "square_skip_gain": square_skip_gain, "mean_step_bias": mean_step_bias, "square_step_bias": square_step_bias}


norm_eps = 1e-05
first_beta = 0.9
second_beta = 0.999
adam_eps = 1e-08
highest = lax.Precision.HIGHEST

def pre_norm(values, gain):
    return values * lax.rsqrt(lax.optimization_barrier(jnp.mean(values * values, axis=-1, keepdims=True)) + norm_eps) * gain

def mixer_front(projected, tail, seg_ext, conv_taps, conv_bias, step_bias, decay_log, skip_gain):
    count = projected.shape[0]
    blocks = count // GROUP
    zgate = projected[:, :INNER]
    xbc = projected[:, INNER:INNER + XBC]
    step_raw = projected[:, INNER + XBC:]
    own_seg = seg_ext[CONV - 1:]
    joined = jnp.concatenate([tail, xbc], axis=0)
    conv = jnp.zeros_like(xbc) + conv_bias[None, :]
    for offset in range(CONV):
        same = (seg_ext[offset:offset + count] == own_seg).astype(jnp.float32)
        conv = conv + conv_taps[offset][None, :] * joined[offset:offset + count] * same[:, None]
    act = jax.nn.silu(conv)
    values = act[:, :INNER].reshape(count, HEADS, HEAD_DIM)
    keys = act[:, INNER:INNER + STATE].reshape(blocks, GROUP, STATE)
    queries_flat = act[:, INNER + STATE:]
    queries = queries_flat.reshape(blocks, GROUP, STATE)
    delta = jax.nn.softplus(step_raw + step_bias[None, :])
    logdec = -delta * jnp.exp(decay_log)[None, :]
    cumul = jnp.cumsum(logdec.reshape(blocks, GROUP, HEADS), axis=1)
    seg_blocks = own_seg.reshape(blocks, GROUP)
    before = jnp.concatenate([seg_ext[CONV - 2:CONV - 1], seg_blocks[:-1, -1]])
    spots = jnp.arange(GROUP)
    causal = (spots[:, None] >= spots[None, :])[None] & (seg_blocks[:, :, None] == seg_blocks[:, None, :])
    causal = causal[..., None]
    diff = cumul[:, :, None, :] - cumul[:, None, :, :]
    decay = jnp.where(causal, jnp.exp(jnp.where(causal, diff, 0.0)), 0.0)
    scores = jnp.einsum('cin,cjn->cij', queries, keys, precision=highest)
    weighted = values.reshape(blocks, GROUP, HEADS, HEAD_DIM) * delta.reshape(blocks, GROUP, HEADS)[..., None]
    intra = jnp.einsum('cijh,cjhp->cihp', decay * scores[..., None], weighted, precision=highest)
    last_seg = seg_blocks[:, -1:]
    to_end = jnp.where((seg_blocks == last_seg)[..., None], jnp.exp(cumul[:, -1:, :] - cumul), 0.0)
    states = jnp.einsum('cjhp,cjn->chpn', weighted * to_end[..., None], keys, precision=highest)
    enter = jnp.where((seg_blocks == before[:, None])[..., None], jnp.exp(cumul), 0.0)
    whole = enter[:, -1, :]

    def advance(carry, item):
        carried, passed = carry
        factor, fresh = item
        return ((factor[:, None, None] * carried + fresh, factor * passed), (carried, passed))
    start = (jnp.zeros((HEADS, HEAD_DIM, STATE), jnp.float32), jnp.ones((HEADS,), jnp.float32))
    (carried, passed), (starts, factors) = lax.scan(advance, start, (whole, states))
    inter = enter[..., None] * jnp.einsum('cin,chpn->cihp', queries, starts, precision=highest)
    mixed = (intra + inter).reshape(count, HEADS, HEAD_DIM) + skip_gain[None, :, None] * values
    reach = (enter * factors[:, None, :]).reshape(count, HEADS)
    return (mixed, queries_flat, reach, zgate, carried, passed)

def mixer_back(mixed, queries, reach, zgate, incoming, gain_gated):
    count = mixed.shape[0]
    carried_in = jnp.einsum('tn,hpn->thp', queries, incoming, precision=highest)
    full = (mixed + reach[..., None] * carried_in).reshape(count, INNER)
    gated = full * jax.nn.silu(zgate)
    return pre_norm(gated, gain_gated)

def adamw(weight, grad, mean, square, rate, decay):
    new_mean = first_beta * mean + (1.0 - first_beta) * grad
    new_square = second_beta * square + (1.0 - second_beta) * grad * grad
    corrected = new_mean / (1.0 - first_beta ** STEP)
    spread = jnp.sqrt(new_square / (1.0 - second_beta ** STEP))
    new_weight = weight * (1.0 - rate * decay) - rate * corrected / (spread + adam_eps)
    return (new_weight, new_mean, new_square)

def reference(hidden, cotangent, segments, weight_in, weight_out, gain_pre, gain_gated, conv_taps, conv_bias, decay_log, skip_gain, step_bias, mean_weight_in, square_weight_in, mean_weight_out, square_weight_out, mean_gain_pre, square_gain_pre, mean_gain_gated, square_gain_gated, mean_conv_taps, square_conv_taps, mean_conv_bias, square_conv_bias, mean_decay_log, square_decay_log, mean_skip_gain, square_skip_gain, mean_step_bias, square_step_bias):
    w_in = weight_in.astype(jnp.bfloat16)
    w_out = weight_out.astype(jnp.bfloat16)
    pre_gain = lax.optimization_barrier(gain_pre.astype(jnp.bfloat16)).astype(jnp.float32)
    gated_gain = lax.optimization_barrier(gain_gated.astype(jnp.bfloat16)).astype(jnp.float32)
    taps = lax.optimization_barrier(conv_taps.astype(jnp.bfloat16)).astype(jnp.float32)
    cbias = lax.optimization_barrier(conv_bias.astype(jnp.bfloat16)).astype(jnp.float32)
    tail_zero = jnp.zeros((CONV - 1, XBC), jnp.float32)
    state_zero = jnp.zeros((HEADS, HEAD_DIM, STATE), jnp.float32)
    lead = jnp.full((CONV - 1,), -1, jnp.int32)

    def one_sequence(carry, item):
        rows_bf, grad_rows, seg_row = item
        rows = rows_bf.astype(jnp.float32)
        normed32, pull_pre = jax.vjp(pre_norm, rows, pre_gain)
        normed = normed32.astype(jnp.bfloat16)
        projected = jnp.dot(normed, w_in, preferred_element_type=jnp.float32).astype(jnp.bfloat16)
        seg_ext = jnp.concatenate([lead, seg_row.astype(jnp.int32)])

        def mixer(proj32, taps32, bias32, sbias, dlog, skip, gain):
            mixed, queries, reach, zgate, unused_state, unused_decay = mixer_front(proj32, tail_zero, seg_ext, taps32, bias32, sbias, dlog, skip)
            return mixer_back(mixed, queries, reach, zgate, state_zero, gain)
        inner32, pull_mix = jax.vjp(mixer, projected.astype(jnp.float32), taps, cbias, step_bias, decay_log, skip_gain, gated_gain)
        inner = inner32.astype(jnp.bfloat16)
        result = (rows + jnp.dot(inner, w_out, preferred_element_type=jnp.float32)).astype(jnp.bfloat16)
        grad_wout = jnp.dot(inner.T, grad_rows, preferred_element_type=jnp.float32)
        inner_grad = jnp.dot(grad_rows, w_out.T, preferred_element_type=jnp.float32)
        proj_grad32, grad_taps, grad_cbias, grad_sbias, grad_dlog, grad_skip, grad_gated = pull_mix(inner_grad)
        proj_grad = proj_grad32.astype(jnp.bfloat16)
        grad_win = jnp.dot(normed.T, proj_grad, preferred_element_type=jnp.float32)
        normed_grad = jnp.dot(proj_grad, w_in.T, preferred_element_type=jnp.float32)
        grad_rows_in, grad_pre = pull_pre(normed_grad)
        rows_grad = grad_rows.astype(jnp.float32) + grad_rows_in
        fresh = (grad_win, grad_wout, grad_pre, grad_gated, grad_taps, grad_cbias, grad_dlog, grad_skip, grad_sbias)
        carry = tuple((total + part for total, part in zip(carry, fresh)))
        return (carry, (result, rows_grad))
    start = (jnp.zeros_like(weight_in), jnp.zeros_like(weight_out), jnp.zeros_like(gain_pre), jnp.zeros_like(gain_gated), jnp.zeros_like(conv_taps), jnp.zeros_like(conv_bias), jnp.zeros_like(decay_log), jnp.zeros_like(skip_gain), jnp.zeros_like(step_bias))
    grads, (output, input_grad) = lax.scan(one_sequence, start, (hidden, cotangent, segments))
    weights = (weight_in, weight_out, gain_pre, gain_gated, conv_taps, conv_bias, decay_log, skip_gain, step_bias)
    means = (mean_weight_in, mean_weight_out, mean_gain_pre, mean_gain_gated, mean_conv_taps, mean_conv_bias, mean_decay_log, mean_skip_gain, mean_step_bias)
    squares = (square_weight_in, square_weight_out, square_gain_pre, square_gain_gated, square_conv_taps, square_conv_bias, square_decay_log, square_skip_gain, square_step_bias)
    rates = (0.01, 0.01, 0.1, 0.1, 0.1, 0.1, 0.1, 0.1, 0.1)
    decays = (0.1, 0.1, 0.0, 0.0, 0.0, 0.0, 0.0, 0.0, 0.0)
    upd = [adamw(weights[index], grads[index], means[index], squares[index], rates[index], decays[index]) for index in range(9)]
    return (output, input_grad, grads[0], grads[1], grads[2], grads[3], grads[4], grads[5], grads[6], grads[7], grads[8], upd[0][0], upd[1][0], upd[2][0], upd[3][0], upd[4][0], upd[5][0], upd[6][0], upd[7][0], upd[8][0], upd[0][1], upd[1][1], upd[2][1], upd[3][1], upd[4][1], upd[5][1], upd[6][1], upd[7][1], upd[8][1], upd[0][2], upd[1][2], upd[2][2], upd[3][2], upd[4][2], upd[5][2], upd[6][2], upd[7][2], upd[8][2])
```

```python
import functools

import jax
import jax.numpy as jnp
from jax import lax
from jax.experimental import pallas as pl
from jax.experimental.pallas import tpu as pltpu
from jax.sharding import PartitionSpec as P

INNER = 3072
HEADS = 48
HEAD_DIM = 64
STATE = 128
CONV = 4
GROUP = 128
STEP = 4
XBC = 3328

norm_eps = 1e-05
first_beta = 0.9
second_beta = 0.999
adam_eps = 1e-08
HIGHEST = lax.Precision.HIGHEST
BOTH = ("dp", "seq")

HG = 8
CG = HG * HEAD_DIM
F32 = jnp.float32
BF = jnp.bfloat16
NEG = -1e30


def dot(a, b, ca=1, cb=0, precision=None):
    return lax.dot_general(
        a, b, (((ca,), (cb,)), ((), ())), precision=precision, preferred_element_type=F32
    )


def low_lanes(rows):
    return lax.broadcasted_iota(jnp.int32, (rows, 2 * HEAD_DIM), 1) < HEAD_DIM


def shifted(block, by, rows):
    if by % 8 == 0:
        return block[by : by + rows]
    return pltpu.roll(block, block.shape[0] - by, 0)[:rows]


def conv_block(joined, base, lanes, tb_ref, cm):
    block = joined[pl.ds(base, GROUP + 8), lanes]
    total = tb_ref[4:5, lanes] + jnp.zeros((GROUP, 1), F32)
    for k in range(CONV):
        total = total + tb_ref[k : k + 1, lanes] * (shifted(block, 5 + k, GROUP) * cm[:, k : k + 1])
    return total


def fill_joined(joined, tail_ref, x_ref):
    joined[0:8, :] = tail_ref[...].astype(F32)
    joined[8:, :] = x_ref[...].astype(F32)


def bias_of(cm_ref, srow_ref, c, base, turned):
    seg_col = cm_ref[pl.ds(base, GROUP), 6:7]
    seg_row = srow_ref[c, 0:1, :]
    down = lax.broadcasted_iota(jnp.int32, (GROUP, GROUP), 0)
    across = lax.broadcasted_iota(jnp.int32, (GROUP, GROUP), 1)
    order = (across >= down) if turned else (down >= across)
    return jnp.where(order & (seg_col == seg_row), 0.0, NEG)


def front_kernel(
    x_ref, kq_ref, tailx_ref, tailkq_ref, tbx_ref, tbkq_ref, dcol_ref, ccol_ref, crow_ref, cm_ref, srow_ref,
    y_ref, reach_ref, q_ref, car_ref, pas_ref,
    joined, joinedkq, kt_s, q_s, s_s, bias_s, wte_s, inter_s, state_s, fac_s, whole_s,
):
    count = x_ref.shape[0]
    blocks = count // GROUP
    lo = low_lanes(GROUP)

    @pl.when(pl.program_id(0) == 0)
    def _():
        fill_joined(joinedkq, tailkq_ref, kq_ref)

        @pl.loop(0, blocks)
        def _(c):
            base = pl.multiple_of(c * GROUP, GROUP)
            cm = cm_ref[pl.ds(base, GROUP), :]
            parts = []
            for half in range(2):
                conv = conv_block(joinedkq, base, slice(half * STATE, half * STATE + STATE), tbkq_ref, cm)
                parts.append(conv * jax.nn.sigmoid(conv))
            keys, queries = parts
            kt_s[c] = keys.T.astype(BF)
            q_s[c] = queries.astype(BF)
            q_ref[pl.ds(base, GROUP), :] = queries.astype(BF)
            s_s[c] = dot(queries, keys, 1, 1, HIGHEST)
            bias_s[c] = bias_of(cm_ref, srow_ref, c, base, False)

    fill_joined(joined, tailx_ref, x_ref)
    state_s[...] = jnp.zeros_like(state_s)
    fac_s[...] = jnp.ones_like(fac_s)

    @pl.loop(0, blocks)
    def _(c):
        base = pl.multiple_of(c * GROUP, GROUP)
        rows = pl.ds(base, GROUP)
        cm = cm_ref[rows, :]
        enter_mask, end_mask = cm[:, 4:5], cm[:, 5:6]
        bias, scores = bias_s[c], s_s[c]
        dcol, ccol, crow = dcol_ref[0, rows, :], ccol_ref[0, rows, :], crow_ref[0, c]
        inter_s[...] = dot(q_s[c], state_s[...].astype(BF))
        for p in range(HG // 2):
            lanes = slice(p * 128, p * 128 + 128)
            conv = conv_block(joined, base, lanes, tbx_ref, cm)
            x = conv * jax.nn.sigmoid(conv)
            cum = [jnp.broadcast_to(ccol[:, h : h + 1], (GROUP, GROUP)) for h in (2 * p, 2 * p + 1)]
            cexp = jnp.where(lo, cum[0], cum[1])
            dexp = jnp.where(lo, dcol[:, 2 * p : 2 * p + 1], dcol[:, 2 * p + 1 : 2 * p + 2])
            w = x * dexp
            wb = w.astype(BF)
            enter = enter_mask * jnp.exp(cexp)
            wte_s[:, lanes] = (w * (end_mask * jnp.exp(cexp[GROUP - 1 :] - cexp))).astype(BF)
            mats = [
                (jnp.exp(cum[i] - crow[2 * p + i : 2 * p + i + 1] + bias) * scores).astype(BF)
                for i in range(2)
            ]
            zero = jnp.zeros_like(wb)
            spread = jnp.concatenate([jnp.where(lo, wb, zero), jnp.where(lo, zero, wb)], axis=0)
            y = dot(jnp.concatenate(mats, axis=1), spread)
            y_ref[rows, lanes] = y + enter * inter_s[:, lanes] + tbx_ref[5:6, lanes] * x
            reach_ref[rows, lanes] = (enter * fac_s[0:1, lanes]).astype(BF)
            whole_s[0:1, lanes] = enter[GROUP - 1 :]
        state_s[...] = whole_s[0:1, :] * state_s[...] + dot(kt_s[c], wte_s[...])
        fac_s[0:1, :] = fac_s[0:1, :] * whole_s[0:1, :]

    car_ref[...] = state_s[...].astype(BF)
    pas_ref[...] = fac_s[...]


def spec(shape, index=None, **kw):
    if index is None:
        index = lambda *_: (0,) * len(shape)
    return pl.BlockSpec(shape, index, **kw)


def params(**kw):
    return pltpu.CompilerParams(vmem_limit_bytes=60 << 20, **kw)


def front(xz, xoff, tail, tb, dcol, ccol, crow, cm, srow):
    count = xz.shape[0]
    blocks = count // GROUP
    steps = HEADS // HG
    vm = pltpu.VMEM
    return pl.pallas_call(
        front_kernel,
        grid=(steps,),
        out_shape=(
            jax.ShapeDtypeStruct((count, INNER), F32),
            jax.ShapeDtypeStruct((count, INNER), BF),
            jax.ShapeDtypeStruct((count, STATE), BF),
            jax.ShapeDtypeStruct((STATE, INNER), BF),
            jax.ShapeDtypeStruct((8, INNER), F32),
        ),
        in_specs=[
            spec((count, CG), lambda g: (0, xoff // CG + g)),
            spec((count, 2 * STATE), lambda g: (0, (xoff + INNER) // (2 * STATE))),
            spec((8, CG), lambda g: (0, g)),
            spec((8, 2 * STATE), lambda g: (0, INNER // (2 * STATE))),
            spec((8, CG), lambda g: (0, g)),
            spec((8, 2 * STATE), lambda g: (0, INNER // (2 * STATE))),
            spec((1, count, HG), lambda g: (g, 0, 0)),
            spec((1, count, HG), lambda g: (g, 0, 0)),
            spec((1, blocks, HG, GROUP), lambda g: (g, 0, 0, 0)),
            spec((count + 8, 8)),
            spec((blocks, 8, GROUP)),
        ],
        out_specs=(
            spec((count, CG), lambda g: (0, g)),
            spec((count, CG), lambda g: (0, g)),
            spec((count, STATE)),
            spec((STATE, CG), lambda g: (0, g)),
            spec((8, CG), lambda g: (0, g)),
        ),
        scratch_shapes=[
            vm((count + 8, CG), F32),
            vm((count + 8, 2 * STATE), F32),
            vm((blocks, STATE, GROUP), BF),
            vm((blocks, GROUP, STATE), BF),
            vm((blocks, GROUP, GROUP), F32),
            vm((blocks, GROUP, GROUP), F32),
            vm((GROUP, CG), BF),
            vm((GROUP, CG), F32),
            vm((STATE, CG), F32),
            vm((8, CG), F32),
            vm((8, CG), F32),
        ],
        compiler_params=params(),
        name="mixer_front",
    )(xz, xz, tail, tail, tb, tb, dcol, ccol, crow, cm, srow)


def middle_kernel(
    y_ref, reach_ref, q_ref, inc_ref, z_ref, hid_ref, cot_ref, gain_ref, wout_ref,
    out_ref, inner_ref, dy_ref, dz_ref, ginc_ref, ggain_ref,
):
    @pl.when(pl.program_id(0) == 0)
    def _():
        ginc_ref[...] = jnp.zeros_like(ginc_ref)
        ggain_ref[...] = jnp.zeros_like(ggain_ref)

    gain = gain_ref[0:1, :]
    reach = reach_ref[...].astype(F32)
    full = y_ref[...] + reach * dot(q_ref[...], inc_ref[...])
    z = z_ref[...].astype(F32)
    sg = jax.nn.sigmoid(z)
    gated = full * (z * sg)
    scale = lax.rsqrt(jnp.mean(gated * gated, axis=1, keepdims=True) + norm_eps)
    unit = gated * scale
    inner = (unit * gain).astype(BF)
    inner_ref[...] = inner
    out_ref[...] = (hid_ref[...].astype(F32) + dot(inner, wout_ref[...])).astype(BF)
    grad = dot(cot_ref[...], wout_ref[...], 1, 1)
    ggain_ref[0:1, :] += jnp.sum(grad * unit, axis=0, keepdims=True)
    grad = grad * gain
    grad = scale * (grad - unit * jnp.mean(grad * unit, axis=1, keepdims=True))
    dz_ref[...] = (grad * full * (sg * (1.0 + z * (1.0 - sg)))).astype(BF)
    dyb = (grad * (z * sg)).astype(BF)
    dy_ref[...] = dyb
    dy = dyb.astype(F32)
    ginc_ref[...] += dot(q_ref[...].astype(F32).T.astype(BF), (dy * reach).astype(BF))


def middle(y, reach, q, incoming, proj, hid, cot, gain, wout):
    count, width = hid.shape
    blocks = count // GROUP
    row = lambda w: spec((GROUP, w), lambda c: (c, 0))
    once = dict(pipeline_mode=pl.Buffered(1))
    return pl.pallas_call(
        middle_kernel,
        grid=(blocks,),
        out_shape=(
            jax.ShapeDtypeStruct((count, width), BF),
            jax.ShapeDtypeStruct((count, INNER), BF),
            jax.ShapeDtypeStruct((count, INNER), BF),
            jax.ShapeDtypeStruct((count, INNER), BF),
            jax.ShapeDtypeStruct((STATE, INNER), F32),
            jax.ShapeDtypeStruct((8, INNER), F32),
        ),
        in_specs=[
            row(INNER), row(INNER), row(STATE), spec((STATE, INNER)), row(INNER), row(width), row(width),
            spec((8, INNER)), spec((INNER, width), **once),
        ],
        out_specs=(
            row(width), row(INNER), row(INNER), row(INNER), spec((STATE, INNER)), spec((8, INNER)),
        ),
        compiler_params=params(),
        name="middle",
    )(y, reach, q, incoming, proj, hid, cot, gain, wout)


def back_kernel(
    x_ref, kq_ref, tailx_ref, tailkq_ref, tbx_ref, tbkq_ref, dcol_ref, ccol_ref, crow_ref, cm_ref, srow_ref,
    dy_ref, inc_ref, gcar_ref, one_ref,
    px_ref, r_ref, rr_ref, lt_ref, par_ref, gt_ref, last_ref,
    joined, joinedkq, kqc_s, kt_s, k_s, qt_s, q_s, s_s, bias_s, wb_s, wte_s, kg_s, qh_s, conv_s, hs_s, g_s, whole_s,
    ent_s, e_s, dcs, dst_s, dq_s, dk_s,
):
    count = x_ref.shape[0]
    blocks = count // GROUP
    step = pl.program_id(0)
    lo = low_lanes(GROUP)
    eight = jnp.zeros((8, 128), F32)

    @pl.when(step == 0)
    def _():
        fill_joined(joinedkq, tailkq_ref, kq_ref)
        dst_s[...] = jnp.zeros_like(dst_s)
        dq_s[...] = jnp.zeros_like(dq_s)
        dk_s[...] = jnp.zeros_like(dk_s)

        @pl.loop(0, blocks)
        def _(c):
            base = pl.multiple_of(c * GROUP, GROUP)
            cm = cm_ref[pl.ds(base, GROUP), :]
            parts = []
            for half in range(2):
                conv = conv_block(joinedkq, base, slice(half * STATE, half * STATE + STATE), tbkq_ref, cm)
                kqc_s[pl.ds(base, GROUP), half * STATE : half * STATE + STATE] = conv
                parts.append(conv * jax.nn.sigmoid(conv))
            keys, queries = parts
            k_s[c] = keys.astype(BF)
            kt_s[c] = keys.T.astype(BF)
            q_s[c] = queries.astype(BF)
            qt_s[c] = queries.T.astype(BF)
            s_s[c] = dot(keys, queries, 1, 1, HIGHEST)
            bias_s[c] = bias_of(cm_ref, srow_ref, c, base, True)

    fill_joined(joined, tailx_ref, x_ref)
    par_col = pl.multiple_of(step * CG, CG)
    hs_s[0] = inc_ref[...].astype(F32)

    def expand(ccol, dcol, p):
        cum = [jnp.broadcast_to(ccol[:, h : h + 1], (GROUP, GROUP)) for h in (2 * p, 2 * p + 1)]
        dexp = jnp.where(lo, dcol[:, 2 * p : 2 * p + 1], dcol[:, 2 * p + 1 : 2 * p + 2])
        return cum, jnp.where(lo, cum[0], cum[1]), dexp

    @pl.loop(0, blocks)
    def _(c):
        base = pl.multiple_of(c * GROUP, GROUP)
        rows = pl.ds(base, GROUP)
        cm = cm_ref[rows, :]
        dcol, ccol = dcol_ref[0, rows, :], ccol_ref[0, rows, :]
        for p in range(HG // 2):
            lanes = slice(p * 128, p * 128 + 128)
            conv = conv_block(joined, base, lanes, tbx_ref, cm)
            conv_s[rows, lanes] = conv
            cum, cexp, dexp = expand(ccol, dcol, p)
            w = conv * jax.nn.sigmoid(conv) * dexp
            wb_s[rows, lanes] = w.astype(BF)
            end = cm[:, 5:6] * jnp.exp(cexp[GROUP - 1 :] - cexp)
            wte_s[rows, lanes] = (w * end).astype(BF)
            whole_s[c, 0:1, lanes] = cm[GROUP - 1 :, 4:5] * jnp.exp(cexp[GROUP - 1 :])
        hs_s[c + 1] = whole_s[c, 0:1, :] * hs_s[c] + dot(kt_s[c], wte_s[rows, :])

    g_s[...] = gcar_ref[...].astype(F32)
    dcs[0:8, :] = jnp.zeros((8, CG), F32)
    dcs[count + 8 :, :] = jnp.zeros((8, CG), F32)
    par_ref[:, pl.ds(par_col, CG)] = jnp.zeros((8, CG), F32)

    @pl.loop(0, blocks)
    def _(i):
        c = blocks - 1 - i
        base = pl.multiple_of(c * GROUP, GROUP)
        rows = pl.ds(base, GROUP)
        cm = cm_ref[rows, :]
        bias, scores = bias_s[c], s_s[c]
        dcol, ccol, crow = dcol_ref[0, rows, :], ccol_ref[0, rows, :], crow_ref[0, c]
        gb = g_s[...].astype(BF)
        kg_s[...] = dot(k_s[c], gb)
        hb = hs_s[c].astype(BF)
        qh_s[...] = dot(q_s[c], hb)
        gh = whole_s[c, 0:1, :] * jnp.sum(g_s[...] * hs_s[c], axis=0, keepdims=True)
        lane = lax.broadcasted_iota(jnp.int32, (GROUP, GROUP), 1)
        cols = jnp.zeros((GROUP, GROUP), F32)
        for p in range(HG // 2):
            lanes = slice(p * 128, p * 128 + 128)
            conv = conv_s[rows, lanes]
            sg = jax.nn.sigmoid(conv)
            x = conv * sg
            cum, cexp, dexp = expand(ccol, dcol, p)
            dyb = dy_ref[rows, lanes]
            dy = dyb.astype(F32)
            wb = wb_s[rows, lanes]
            zero = jnp.zeros_like(dyb)
            spread = jnp.concatenate([jnp.where(lo, dyb, zero), jnp.where(lo, zero, dyb)], axis=0)
            dmat = dot(wb, spread, 1, 1)
            decay = [jnp.exp(crow[2 * p + i : 2 * p + i + 1] - cum[i] + bias) for i in range(2)]
            dst_s[c] += dmat[:, :GROUP] * decay[0] + dmat[:, GROUP:] * decay[1]
            mats = [d * scores for d in decay]
            for i in range(2):
                pairs = dmat[:, i * GROUP : (i + 1) * GROUP] * mats[i]
                cols = jnp.where(lane == 2 * p + i, jnp.sum(pairs, axis=1, keepdims=True), cols)
                rr_ref[0, c, 2 * p + i : 2 * p + i + 1, :] = jnp.sum(pairs, axis=0, keepdims=True)
            mats = jnp.concatenate([m.astype(BF) for m in mats], axis=1)
            end = cm[:, 5:6] * jnp.exp(cexp[GROUP - 1 :] - cexp)
            enter = cm[:, 4:5] * jnp.exp(cexp)
            kge = end * kg_s[:, lanes]
            dw = dot(mats, spread) + kge
            edy = enter * dy
            ent_s[:, lanes] = edy.astype(BF)
            kge = wb.astype(F32) * kge
            lt_ref[c, 0:1, pl.ds(par_col + p * 128, 128)] = gh[:, lanes] + jnp.sum(kge, axis=0, keepdims=True)
            skip = tbx_ref[5:6, lanes]
            skx = dy * x
            for n, e in enumerate((edy * qh_s[:, lanes] - kge, x * dw)):
                high = e.astype(BF)
                e_s[0, :, n * CG + p * 128 : n * CG + p * 128 + 128] = high
                e_s[1, :, n * CG + p * 128 : n * CG + p * 128 + 128] = (e - high.astype(F32)).astype(BF)
            dconv = (dexp * dw + skip * dy) * (sg * (1.0 + conv * (1.0 - sg)))
            dcs[pl.ds(base + 8, GROUP), lanes] = dconv
            block = joined[pl.ds(base, GROUP + 8), lanes]
            sums = [
                jnp.sum(dconv * (shifted(block, 5 + k, GROUP) * cm[:, k : k + 1]), axis=0, keepdims=True)
                for k in range(CONV)
            ]
            sums += [jnp.sum(dconv, axis=0, keepdims=True), jnp.sum(skx, axis=0, keepdims=True)]
            par_ref[:, pl.ds(par_col + p * 128, 128)] += jnp.concatenate(sums + [eight[:2]], axis=0)
        entb = ent_s[...]
        dq_s[c] += dot(entb, hb, 1, 1)
        dk_s[c] += dot(wte_s[rows, :], gb, 1, 1)
        g_s[...] = whole_s[c, 0:1, :] * g_s[...] + dot(qt_s[c], entb)
        r_ref[0, rows, :] = dot(e_s[0], one_ref[...]) + dot(e_s[1], one_ref[...]) - cols[:, : 2 * HG]

    def unconv(dcs_ref, tb_ref, width, col):
        for q in range(width // 128):
            lanes = slice(q * 128, q * 128 + 128)
            cols = pl.ds(col + q * 128, 128)

            def pull(start, rows, cm_start):
                block = dcs_ref[pl.ds(start, rows + 8), lanes]
                cm = cm_ref[pl.ds(cm_start, rows + 8), :]
                total = jnp.zeros((rows, 128), F32)
                for k in range(CONV):
                    total = total + tb_ref[k : k + 1, lanes] * shifted(block * cm[:, k : k + 1], 3 - k, rows)
                return total

            @pl.loop(0, blocks)
            def _(c):
                base = pl.multiple_of(c * GROUP, GROUP)
                got = pull(base + 8, GROUP, base)
                px_ref[pl.ds(base, GROUP), cols] = got.astype(BF)
                last_ref[:, cols] = got[GROUP - 8 :]

            block = jnp.concatenate([jnp.zeros((8, 128), F32), dcs_ref[8:16, lanes]], axis=0)
            cm = jnp.concatenate([jnp.zeros((8, 8), F32), cm_ref[0:8, :]], axis=0)
            total = jnp.zeros((8, 128), F32)
            for k in range(CONV):
                total = total + tb_ref[k : k + 1, lanes] * shifted(block * cm[:, k : k + 1], 3 - k, 8)
            gt_ref[:, cols] = total

    unconv(dcs, tbx_ref, CG, par_col)

    @pl.when(step == pl.num_programs(0) - 1)
    def _():
        par_ref[:, INNER:] = jnp.zeros((8, 2 * STATE), F32)

        @pl.loop(0, blocks)
        def _(c):
            base = pl.multiple_of(c * GROUP, GROUP)
            rows = pl.ds(base, GROUP)
            cm = cm_ref[rows, :]
            dst = dst_s[c]
            dk = dk_s[c] + dot(dst.astype(BF), q_s[c])
            dq = dq_s[c] + dot(dst.T.astype(BF), k_s[c])
            for half, grad in enumerate((dk, dq)):
                lanes = slice(half * STATE, half * STATE + STATE)
                conv = kqc_s[rows, lanes]
                sg = jax.nn.sigmoid(conv)
                dconv = grad * (sg * (1.0 + conv * (1.0 - sg)))
                dcs[pl.ds(base + 8, GROUP), lanes] = dconv
                block = joinedkq[pl.ds(base, GROUP + 8), lanes]
                sums = [
                    jnp.sum(dconv * (shifted(block, 5 + k, GROUP) * cm[:, k : k + 1]), axis=0, keepdims=True)
                    for k in range(CONV)
                ]
                sums += [jnp.sum(dconv, axis=0, keepdims=True)]
                par_ref[:, INNER + half * STATE : INNER + half * STATE + STATE] += jnp.concatenate(
                    sums + [eight[:3]], axis=0
                )

        unconv(dcs, tbkq_ref, 2 * STATE, INNER)


def back(xz, xoff, tail, tb, dcol, ccol, crow, cm, srow, dy, incoming, gcar, one):
    count = xz.shape[0]
    blocks = count // GROUP
    steps = HEADS // HG
    vm = pltpu.VMEM
    return pl.pallas_call(
        back_kernel,
        grid=(steps,),
        out_shape=(
            jax.ShapeDtypeStruct((count, XBC), BF),
            jax.ShapeDtypeStruct((steps, count, 2 * HG), F32),
            jax.ShapeDtypeStruct((steps, blocks, HG, GROUP), F32),
            jax.ShapeDtypeStruct((blocks, 8, INNER), F32),
            jax.ShapeDtypeStruct((8, XBC), F32),
            jax.ShapeDtypeStruct((8, XBC), F32),
            jax.ShapeDtypeStruct((8, XBC), F32),
        ),
        in_specs=[
            spec((count, CG), lambda g: (0, xoff // CG + g)),
            spec((count, 2 * STATE), lambda g: (0, (xoff + INNER) // (2 * STATE))),
            spec((8, CG), lambda g: (0, g)),
            spec((8, 2 * STATE), lambda g: (0, INNER // (2 * STATE))),
            spec((8, CG), lambda g: (0, g)),
            spec((8, 2 * STATE), lambda g: (0, INNER // (2 * STATE))),
            spec((1, count, HG), lambda g: (g, 0, 0)),
            spec((1, count, HG), lambda g: (g, 0, 0)),
            spec((1, blocks, HG, GROUP), lambda g: (g, 0, 0, 0)),
            spec((count + 8, 8)),
            spec((blocks, 8, GROUP)),
            spec((count, CG), lambda g: (0, g)),
            spec((STATE, CG), lambda g: (0, g)),
            spec((STATE, CG), lambda g: (0, g)),
            spec((2 * CG, 2 * HG)),
        ],
        out_specs=(
            spec((count, XBC)),
            spec((1, count, 2 * HG), lambda g: (g, 0, 0)),
            spec((1, blocks, HG, GROUP), lambda g: (g, 0, 0, 0)),
            spec((blocks, 8, INNER)),
            spec((8, XBC)),
            spec((8, XBC)),
            spec((8, XBC)),
        ),
        scratch_shapes=[
            vm((count + 8, CG), F32),
            vm((count + 8, 2 * STATE), F32),
            vm((count, 2 * STATE), F32),
            vm((blocks, STATE, GROUP), BF),
            vm((blocks, GROUP, STATE), BF),
            vm((blocks, STATE, GROUP), BF),
            vm((blocks, GROUP, STATE), BF),
            vm((blocks, GROUP, GROUP), F32),
            vm((blocks, GROUP, GROUP), F32),
            vm((count, CG), BF),
            vm((count, CG), BF),
            vm((GROUP, CG), F32),
            vm((GROUP, CG), F32),
            vm((count, CG), F32),
            vm((blocks + 1, STATE, CG), F32),
            vm((STATE, CG), F32),
            vm((blocks, 8, CG), F32),
            vm((GROUP, CG), BF),
            vm((2, GROUP, 2 * CG), BF),
            vm((count + 16, CG), F32),
            vm((blocks, GROUP, GROUP), F32),
            vm((blocks, GROUP, STATE), F32),
            vm((blocks, GROUP, STATE), F32),
        ],
        compiler_params=params(),
        name="mixer_back",
    )(xz, xz, tail, tail, tb, tb, dcol, ccol, crow, cm, srow, dy, incoming, gcar, one)


def passed_along(shard, axis, by):
    count = lax.axis_size(axis)
    pairs = [(i, i + by) for i in range(count) if 0 <= i + by < count]
    return lax.ppermute(shard, axis, pairs)


def chained(own, factor, axis, by):
    got = jnp.zeros(own.shape, BF)
    for i in range(lax.axis_size(axis) - 1):
        sent = own if i == 0 else own.astype(F32) + factor * got.astype(F32)
        got = passed_along(sent.astype(BF), axis, by)
    return got


def adamw(weight, grad, mean, square, rate, decay):
    new_mean = first_beta * mean + (1.0 - first_beta) * grad
    new_square = second_beta * square + (1.0 - second_beta) * grad * grad
    corrected = new_mean / (1.0 - first_beta**STEP)
    spread = jnp.sqrt(new_square / (1.0 - second_beta**STEP))
    new_weight = weight * (1.0 - rate * decay) - rate * corrected / (spread + adam_eps)
    return (new_weight, new_mean, new_square)


def prepare(step_raw, seg_ext, step_bias, decay_log):
    count = step_raw.shape[0]
    blocks, steps = count // GROUP, HEADS // HG
    delta = jax.nn.softplus(step_raw + step_bias[None, :])
    logdec = -delta * jnp.exp(decay_log)[None, :]
    lower = jnp.tril(jnp.ones((GROUP, GROUP), F32))
    cum = jnp.einsum("ij,cjh->cih", lower, logdec.reshape(blocks, GROUP, HEADS), precision=HIGHEST)
    own = seg_ext[CONV - 1 :]
    seg_blocks = own.reshape(blocks, GROUP)
    before = jnp.concatenate([seg_ext[CONV - 2 : CONV - 1], seg_blocks[:-1, -1]])
    columns = [seg_ext[k : k + count] == own for k in range(CONV)]
    columns += [(seg_blocks == before[:, None]).reshape(count), (seg_blocks == seg_blocks[:, -1:]).reshape(count)]
    columns = [c.astype(F32) for c in columns] + [own.astype(F32), jnp.zeros((count,), F32)]
    cm = jnp.pad(jnp.stack(columns, axis=1), ((0, 8), (0, 0)))
    srow = jnp.broadcast_to(seg_blocks.astype(F32)[:, None, :], (blocks, 8, GROUP))
    dcol = delta.reshape(count, steps, HG).transpose(1, 0, 2)
    ccol = cum.reshape(count, steps, HG).transpose(1, 0, 2)
    crow = cum.reshape(blocks, GROUP, steps, HG).transpose(2, 0, 3, 1)
    return delta, logdec, (dcol, ccol, crow, cm, srow)


def shards(
    hidden,
    cotangent,
    segments,
    weight_in,
    weight_out,
    gain_pre,
    gain_gated,
    conv_taps,
    conv_bias,
    decay_log,
    skip_gain,
    step_bias,
    mean_weight_in,
    square_weight_in,
    mean_weight_out,
    square_weight_out,
    mean_gain_pre,
    square_gain_pre,
    mean_gain_gated,
    square_gain_gated,
    mean_conv_taps,
    square_conv_taps,
    mean_conv_bias,
    square_conv_bias,
    mean_decay_log,
    square_decay_log,
    mean_skip_gain,
    square_skip_gain,
    mean_step_bias,
    square_step_bias,
):
    piece = hidden.shape[1]
    blocks, steps = piece // GROUP, HEADS // HG
    devices = lax.axis_size("dp") * lax.axis_size("seq")
    offset = lax.axis_index("seq") * piece
    lead = jnp.full((CONV - 1,), -1, jnp.int32)
    seg_ext = lax.dynamic_slice_in_dim(jnp.concatenate([lead, segments[0]]), offset, piece + CONV - 1)

    sizes = (gain_pre.shape[0], gain_gated.shape[0], conv_taps.size, conv_bias.shape[0])
    small = jnp.concatenate([gain_pre, gain_gated, conv_taps.reshape(-1), conv_bias]).astype(BF)
    small = lax.all_gather(small, BOTH, axis=0).astype(F32)
    w_in = lax.all_gather(weight_in.astype(BF), BOTH, axis=0, tiled=True)
    w_out = lax.all_gather(weight_out.astype(BF), BOTH, axis=0, tiled=True)
    cuts = [0]
    for s in sizes:
        cuts.append(cuts[-1] + s)
    pre_gain, gated_gain, taps, cbias = [small[:, a:b] for a, b in zip(cuts, cuts[1:])]
    pre_gain, gated_gain, cbias = pre_gain.reshape(-1), gated_gain.reshape(-1), cbias.reshape(-1)
    taps = taps.reshape(devices, CONV, -1).transpose(1, 0, 2).reshape(CONV, XBC)

    rows = hidden[0].astype(F32)
    scale = lax.rsqrt(jnp.mean(rows * rows, axis=-1, keepdims=True) + norm_eps)
    normed = (rows * scale * pre_gain).astype(BF)
    proj = jnp.dot(normed, w_in, preferred_element_type=F32).astype(BF)
    tail = passed_along(proj[piece - CONV + 1 :, INNER : INNER + XBC], "seq", 1)
    tail = jnp.pad(tail, ((8 - CONV + 1, 0), (0, 0)))
    skip_lanes = jnp.pad(jnp.repeat(skip_gain, HEAD_DIM), (0, XBC - INNER))
    tb = jnp.concatenate([taps, cbias[None], skip_lanes[None], jnp.zeros((2, XBC), F32)])
    step_raw = proj[:, INNER + XBC :].astype(F32)
    delta, logdec, prepared = prepare(step_raw, seg_ext, step_bias, decay_log)

    mixed, reach, queries, carried, passed = front(proj, INNER, tail, tb, *prepared)
    incoming = chained(carried, passed[:1], "seq", 1)
    gain8 = jnp.broadcast_to(gated_gain[None], (8, INNER))
    output, inner, dy, dz, ginc, ggain = middle(
        mixed, reach, queries, incoming, proj, hidden[0], cotangent[0], gain8, w_out
    )
    grad_gated = ggain[0]
    gcar = chained(ginc, passed[:1], "seq", -1)
    grad_wout = jnp.dot(inner.T, cotangent[0], preferred_element_type=F32)
    group = jnp.arange(2 * CG) // HEAD_DIM
    two = (group[:, None] == jnp.arange(2 * HG)[None, :]).astype(BF)
    px, r, rr, lt, par, gt, last = back(proj, INNER, tail, tb, *prepared, dy, incoming, gcar, two)
    returned = passed_along(gt[8 - CONV + 1 :].astype(BF), "seq", -1).astype(F32)
    patched = (last[8 - CONV + 1 :] + returned).astype(BF)
    px = px.at[piece - CONV + 1 :].set(patched)

    r = r.transpose(1, 0, 2)
    r1, r2 = r[..., :HG].reshape(piece, HEADS), r[..., HG:].reshape(piece, HEADS)
    dcum = r1.reshape(blocks, GROUP, HEADS) + rr.transpose(1, 3, 0, 2).reshape(blocks, GROUP, HEADS)
    ends = jnp.sum(lt[:, 0].reshape(blocks, HEADS, HEAD_DIM), axis=-1)
    upper = jnp.triu(jnp.ones((GROUP, GROUP), F32))
    dlogdec = jnp.einsum("ij,cjh->cih", upper, dcum, precision=HIGHEST) + ends[:, None, :]
    dlogdec = dlogdec.reshape(piece, HEADS)
    dstep = (r2 - jnp.exp(decay_log)[None] * dlogdec) * jax.nn.sigmoid(step_raw + step_bias[None])
    grad_dlog = jnp.sum(dlogdec * logdec, axis=0)
    grad_sbias = jnp.sum(dstep, axis=0)
    grad_skip = jnp.sum(par[5, :INNER].reshape(HEADS, HEAD_DIM), axis=-1)
    grad_taps, grad_cbias = par[:CONV], par[4]

    proj_grad = jnp.concatenate([dz, px, dstep.astype(BF)], axis=1)
    grad_win = jnp.dot(normed.T, proj_grad, preferred_element_type=F32)
    normed_grad = jnp.dot(proj_grad, w_in.T, preferred_element_type=F32)
    unit = rows * scale
    grad_pre = jnp.sum(normed_grad * unit, axis=0)
    pulled = normed_grad * pre_gain
    pulled = scale * (pulled - unit * jnp.mean(pulled * unit, axis=-1, keepdims=True))
    input_grad = cotangent[0].astype(F32) + pulled

    def scattered(total):
        return lax.psum_scatter(total.astype(BF), BOTH, scatter_dimension=0, tiled=True).astype(F32)

    share_in, share_out = scattered(grad_win), scattered(grad_wout)
    smalls = (grad_pre, grad_gated, grad_taps.reshape(-1), grad_cbias, grad_dlog, grad_skip, grad_sbias)
    summed = lax.psum(jnp.concatenate(smalls), BOTH)
    me = lax.axis_index("dp") * lax.axis_size("seq") + lax.axis_index("seq")
    pieces, start = [], 0
    for s in smalls:
        pieces.append(summed[start : start + s.shape[0]])
        start += s.shape[0]
    mine = [lax.dynamic_slice_in_dim(p, me * s, s) for p, s in zip(pieces, sizes) if True]
    own_taps = lax.dynamic_slice_in_dim(
        pieces[2].reshape(CONV, XBC), me * conv_taps.shape[1], conv_taps.shape[1], axis=1
    )
    grads = (share_in, share_out, mine[0], mine[1], own_taps, mine[3], pieces[4], pieces[5], pieces[6])
    weights = (
        weight_in,
        weight_out,
        gain_pre,
        gain_gated,
        conv_taps,
        conv_bias,
        decay_log,
        skip_gain,
        step_bias,
    )
    means = (
        mean_weight_in,
        mean_weight_out,
        mean_gain_pre,
        mean_gain_gated,
        mean_conv_taps,
        mean_conv_bias,
        mean_decay_log,
        mean_skip_gain,
        mean_step_bias,
    )
    squares = (
        square_weight_in,
        square_weight_out,
        square_gain_pre,
        square_gain_gated,
        square_conv_taps,
        square_conv_bias,
        square_decay_log,
        square_skip_gain,
        square_step_bias,
    )
    rates = (0.01, 0.01, 0.1, 0.1, 0.1, 0.1, 0.1, 0.1, 0.1)
    decays = (0.1, 0.1, 0.0, 0.0, 0.0, 0.0, 0.0, 0.0, 0.0)
    updated = [
        adamw(weights[index], grads[index], means[index], squares[index], rates[index], decays[index])
        for index in range(9)
    ]
    new_weights = tuple((entry[0] for entry in updated))
    new_means = tuple((entry[1] for entry in updated))
    new_squares = tuple((entry[2] for entry in updated))
    return (output[None], input_grad[None]) + grads + new_weights + new_means + new_squares


def solution(mesh):
    dp, seq, both = P("dp"), P("seq"), P(BOTH)
    rows, cols, copied = P(BOTH, None), P(None, BOTH), P()
    whole = P("dp", "seq", None)
    kinds = (rows, rows, both, both, cols, both, copied, copied, copied)
    pairs = tuple(kind for kind in kinds for _ in range(2))
    return jax.shard_map(
        shards,
        mesh=mesh,
        in_specs=(whole, whole, P("dp", None)) + kinds + pairs,
        out_specs=(whole, whole) + kinds * 4,
        check_vma=False,
    )
```

```python
import functools

import jax
import jax.numpy as jnp
from jax import lax
from jax.experimental import pallas as pl
from jax.experimental.pallas import tpu as pltpu
from jax.sharding import PartitionSpec as P

INNER = 3072
HEADS = 48
HEAD_DIM = 64
STATE = 128
CONV = 4
GROUP = 128
STEP = 4
XBC = 3328

norm_eps = 1e-05
first_beta = 0.9
second_beta = 0.999
adam_eps = 1e-08
HIGHEST = lax.Precision.HIGHEST
BOTH = ("dp", "seq")

HG = 8
CG = HG * HEAD_DIM
F32 = jnp.float32
BF = jnp.bfloat16
NEG = -1e30


def dot(a, b, ca=1, cb=0, precision=None):
    return lax.dot_general(
        a, b, (((ca,), (cb,)), ((), ())), precision=precision, preferred_element_type=F32
    )


def low_lanes(rows):
    return lax.broadcasted_iota(jnp.int32, (rows, 2 * HEAD_DIM), 1) < HEAD_DIM


def shifted(block, by, rows):
    if by % 8 == 0:
        return block[by : by + rows]
    return pltpu.roll(block, block.shape[0] - by, 0)[:rows]


def conv_block(joined, base, lanes, tb_ref, cm):
    block = joined[pl.ds(base, GROUP + 8), lanes]
    total = tb_ref[4:5, lanes] + jnp.zeros((GROUP, 1), F32)
    for k in range(CONV):
        total = total + tb_ref[k : k + 1, lanes] * (shifted(block, 5 + k, GROUP) * cm[:, k : k + 1])
    return total


def fill_joined(joined, tail_ref, x_ref):
    joined[0:8, :] = tail_ref[...].astype(F32)
    joined[8:, :] = x_ref[...].astype(F32)


def bias_of(cm_ref, srow_ref, c, base, turned):
    seg_col = cm_ref[pl.ds(base, GROUP), 6:7]
    seg_row = srow_ref[c, 0:1, :]
    down = lax.broadcasted_iota(jnp.int32, (GROUP, GROUP), 0)
    across = lax.broadcasted_iota(jnp.int32, (GROUP, GROUP), 1)
    order = (across >= down) if turned else (down >= across)
    return jnp.where(order & (seg_col == seg_row), 0.0, NEG)


def front_kernel(
    x_ref, kq_ref, tailx_ref, tailkq_ref, tbx_ref, tbkq_ref, dcol_ref, ccol_ref, crow_ref, cm_ref, srow_ref,
    y_ref, reach_ref, q_ref, car_ref, pas_ref,
    joined, joinedkq, kt_s, q_s, s_s, bias_s, wte_s, inter_s, state_s, fac_s, whole_s,
):
    count = x_ref.shape[0]
    blocks = count // GROUP
    lo = low_lanes(GROUP)

    @pl.when(pl.program_id(0) == 0)
    def _():
        fill_joined(joinedkq, tailkq_ref, kq_ref)

        @pl.loop(0, blocks)
        def _(c):
            base = pl.multiple_of(c * GROUP, GROUP)
            cm = cm_ref[pl.ds(base, GROUP), :]
            parts = []
            for half in range(2):
                conv = conv_block(joinedkq, base, slice(half * STATE, half * STATE + STATE), tbkq_ref, cm)
                parts.append(conv * jax.nn.sigmoid(conv))
            keys, queries = parts
            kt_s[c] = keys.T.astype(BF)
            q_s[c] = queries.astype(BF)
            q_ref[pl.ds(base, GROUP), :] = queries.astype(BF)
            s_s[c] = dot(queries, keys, 1, 1, HIGHEST)
            bias_s[c] = bias_of(cm_ref, srow_ref, c, base, False)

    fill_joined(joined, tailx_ref, x_ref)
    state_s[...] = jnp.zeros_like(state_s)
    fac_s[...] = jnp.ones_like(fac_s)

    @pl.loop(0, blocks)
    def _(c):
        base = pl.multiple_of(c * GROUP, GROUP)
        rows = pl.ds(base, GROUP)
        cm = cm_ref[rows, :]
        enter_mask, end_mask = cm[:, 4:5], cm[:, 5:6]
        bias, scores = bias_s[c], s_s[c]
        dcol, ccol, crow = dcol_ref[0, rows, :], ccol_ref[0, rows, :], crow_ref[0, c]
        inter_s[...] = dot(q_s[c], state_s[...].astype(BF))
        for p in range(HG // 2):
            lanes = slice(p * 128, p * 128 + 128)
            conv = conv_block(joined, base, lanes, tbx_ref, cm)
            x = conv * jax.nn.sigmoid(conv)
            cum = [jnp.broadcast_to(ccol[:, h : h + 1], (GROUP, GROUP)) for h in (2 * p, 2 * p + 1)]
            cexp = jnp.where(lo, cum[0], cum[1])
            dexp = jnp.where(lo, dcol[:, 2 * p : 2 * p + 1], dcol[:, 2 * p + 1 : 2 * p + 2])
            w = x * dexp
            wb = w.astype(BF)
            enter = enter_mask * jnp.exp(cexp)
            wte_s[:, lanes] = (w * (end_mask * jnp.exp(cexp[GROUP - 1 :] - cexp))).astype(BF)
            mats = [
                (jnp.exp(cum[i] - crow[2 * p + i : 2 * p + i + 1] + bias) * scores).astype(BF)
                for i in range(2)
            ]
            zero = jnp.zeros_like(wb)
            spread = jnp.concatenate([jnp.where(lo, wb, zero), jnp.where(lo, zero, wb)], axis=0)
            y = dot(jnp.concatenate(mats, axis=1), spread)
            y_ref[rows, lanes] = y + enter * inter_s[:, lanes] + tbx_ref[5:6, lanes] * x
            reach_ref[rows, lanes] = (enter * fac_s[0:1, lanes]).astype(BF)
            whole_s[0:1, lanes] = enter[GROUP - 1 :]
        state_s[...] = whole_s[0:1, :] * state_s[...] + dot(kt_s[c], wte_s[...])
        fac_s[0:1, :] = fac_s[0:1, :] * whole_s[0:1, :]

    car_ref[...] = state_s[...].astype(BF)
    pas_ref[...] = fac_s[...]


def spec(shape, index=None, **kw):
    if index is None:
        index = lambda *_: (0,) * len(shape)
    return pl.BlockSpec(shape, index, **kw)


def params(**kw):
    return pltpu.CompilerParams(vmem_limit_bytes=60 << 20, **kw)


def front(xz, xoff, tail, tb, dcol, ccol, crow, cm, srow):
    count = xz.shape[0]
    blocks = count // GROUP
    steps = HEADS // HG
    vm = pltpu.VMEM
    return pl.pallas_call(
        front_kernel,
        grid=(steps,),
        out_shape=(
            jax.ShapeDtypeStruct((count, INNER), F32),
            jax.ShapeDtypeStruct((count, INNER), BF),
            jax.ShapeDtypeStruct((count, STATE), BF),
            jax.ShapeDtypeStruct((STATE, INNER), BF),
            jax.ShapeDtypeStruct((8, INNER), F32),
        ),
        in_specs=[
            spec((count, CG), lambda g: (0, xoff // CG + g)),
            spec((count, 2 * STATE), lambda g: (0, (xoff + INNER) // (2 * STATE))),
            spec((8, CG), lambda g: (0, g)),
            spec((8, 2 * STATE), lambda g: (0, INNER // (2 * STATE))),
            spec((8, CG), lambda g: (0, g)),
            spec((8, 2 * STATE), lambda g: (0, INNER // (2 * STATE))),
            spec((1, count, HG), lambda g: (g, 0, 0)),
            spec((1, count, HG), lambda g: (g, 0, 0)),
            spec((1, blocks, HG, GROUP), lambda g: (g, 0, 0, 0)),
            spec((count + 8, 8)),
            spec((blocks, 8, GROUP)),
        ],
        out_specs=(
            spec((count, CG), lambda g: (0, g)),
            spec((count, CG), lambda g: (0, g)),
            spec((count, STATE)),
            spec((STATE, CG), lambda g: (0, g)),
            spec((8, CG), lambda g: (0, g)),
        ),
        scratch_shapes=[
            vm((count + 8, CG), F32),
            vm((count + 8, 2 * STATE), F32),
            vm((blocks, STATE, GROUP), BF),
            vm((blocks, GROUP, STATE), BF),
            vm((blocks, GROUP, GROUP), F32),
            vm((blocks, GROUP, GROUP), F32),
            vm((GROUP, CG), BF),
            vm((GROUP, CG), F32),
            vm((STATE, CG), F32),
            vm((8, CG), F32),
            vm((8, CG), F32),
        ],
        compiler_params=params(),
        name="mixer_front",
    )(xz, xz, tail, tail, tb, tb, dcol, ccol, crow, cm, srow)


def middle_kernel(
    y_ref, reach_ref, q_ref, inc_ref, z_ref, hid_ref, cot_ref, gain_ref, wout_ref,
    out_ref, inner_ref, dy_ref, dz_ref, ginc_ref, ggain_ref,
):
    @pl.when(pl.program_id(0) == 0)
    def _():
        ginc_ref[...] = jnp.zeros_like(ginc_ref)
        ggain_ref[...] = jnp.zeros_like(ggain_ref)

    gain = gain_ref[0:1, :]
    reach = reach_ref[...].astype(F32)
    full = y_ref[...] + reach * dot(q_ref[...], inc_ref[...])
    z = z_ref[...].astype(F32)
    sg = jax.nn.sigmoid(z)
    gated = full * (z * sg)
    scale = lax.rsqrt(jnp.mean(gated * gated, axis=1, keepdims=True) + norm_eps)
    unit = gated * scale
    inner = (unit * gain).astype(BF)
    inner_ref[...] = inner
    out_ref[...] = (hid_ref[...].astype(F32) + dot(inner, wout_ref[...])).astype(BF)
    grad = dot(cot_ref[...], wout_ref[...], 1, 1)
    ggain_ref[0:1, :] += jnp.sum(grad * unit, axis=0, keepdims=True)
    grad = grad * gain
    grad = scale * (grad - unit * jnp.mean(grad * unit, axis=1, keepdims=True))
    dz_ref[...] = (grad * full * (sg * (1.0 + z * (1.0 - sg)))).astype(BF)
    dyb = (grad * (z * sg)).astype(BF)
    dy_ref[...] = dyb
    dy = dyb.astype(F32)
    ginc_ref[...] += dot(q_ref[...].astype(F32).T.astype(BF), (dy * reach).astype(BF))


def middle(y, reach, q, incoming, proj, hid, cot, gain, wout):
    count, width = hid.shape
    blocks = count // GROUP
    row = lambda w: spec((GROUP, w), lambda c: (c, 0))
    once = dict(pipeline_mode=pl.Buffered(1))
    return pl.pallas_call(
        middle_kernel,
        grid=(blocks,),
        out_shape=(
            jax.ShapeDtypeStruct((count, width), BF),
            jax.ShapeDtypeStruct((count, INNER), BF),
            jax.ShapeDtypeStruct((count, INNER), BF),
            jax.ShapeDtypeStruct((count, INNER), BF),
            jax.ShapeDtypeStruct((STATE, INNER), F32),
            jax.ShapeDtypeStruct((8, INNER), F32),
        ),
        in_specs=[
            row(INNER), row(INNER), row(STATE), spec((STATE, INNER)), row(INNER), row(width), row(width),
            spec((8, INNER)), spec((INNER, width), **once),
        ],
        out_specs=(
            row(width), row(INNER), row(INNER), row(INNER), spec((STATE, INNER)), spec((8, INNER)),
        ),
        compiler_params=params(),
        name="middle",
    )(y, reach, q, incoming, proj, hid, cot, gain, wout)


def back_kernel(
    x_ref, kq_ref, tailx_ref, tailkq_ref, tbx_ref, tbkq_ref, dcol_ref, ccol_ref, crow_ref, cm_ref, srow_ref,
    dy_ref, inc_ref, gcar_ref, one_ref,
    px_ref, r_ref, rr_ref, lt_ref, par_ref, gt_ref, last_ref,
    joined, joinedkq, kqc_s, kt_s, k_s, qt_s, q_s, s_s, bias_s, wb_s, wte_s, kg_s, qh_s, conv_s, hs_s, g_s, whole_s,
    ent_s, e_s, dcs, dst_s, dq_s, dk_s,
):
    count = x_ref.shape[0]
    blocks = count // GROUP
    step = pl.program_id(0)
    lo = low_lanes(GROUP)
    eight = jnp.zeros((8, 128), F32)

    @pl.when(step == 0)
    def _():
        fill_joined(joinedkq, tailkq_ref, kq_ref)
        dst_s[...] = jnp.zeros_like(dst_s)
        dq_s[...] = jnp.zeros_like(dq_s)
        dk_s[...] = jnp.zeros_like(dk_s)

        @pl.loop(0, blocks)
        def _(c):
            base = pl.multiple_of(c * GROUP, GROUP)
            cm = cm_ref[pl.ds(base, GROUP), :]
            parts = []
            for half in range(2):
                conv = conv_block(joinedkq, base, slice(half * STATE, half * STATE + STATE), tbkq_ref, cm)
                kqc_s[pl.ds(base, GROUP), half * STATE : half * STATE + STATE] = conv
                parts.append(conv * jax.nn.sigmoid(conv))
            keys, queries = parts
            k_s[c] = keys.astype(BF)
            kt_s[c] = keys.T.astype(BF)
            q_s[c] = queries.astype(BF)
            qt_s[c] = queries.T.astype(BF)
            s_s[c] = dot(keys, queries, 1, 1, HIGHEST)
            bias_s[c] = bias_of(cm_ref, srow_ref, c, base, True)

    fill_joined(joined, tailx_ref, x_ref)
    par_col = pl.multiple_of(step * CG, CG)
    hs_s[0] = inc_ref[...].astype(F32)

    def expand(ccol, dcol, p):
        cum = [jnp.broadcast_to(ccol[:, h : h + 1], (GROUP, GROUP)) for h in (2 * p, 2 * p + 1)]
        dexp = jnp.where(lo, dcol[:, 2 * p : 2 * p + 1], dcol[:, 2 * p + 1 : 2 * p + 2])
        return cum, jnp.where(lo, cum[0], cum[1]), dexp

    @pl.loop(0, blocks)
    def _(c):
        base = pl.multiple_of(c * GROUP, GROUP)
        rows = pl.ds(base, GROUP)
        cm = cm_ref[rows, :]
        dcol, ccol = dcol_ref[0, rows, :], ccol_ref[0, rows, :]
        for p in range(HG // 2):
            lanes = slice(p * 128, p * 128 + 128)
            conv = conv_block(joined, base, lanes, tbx_ref, cm)
            conv_s[rows, lanes] = conv
            cum, cexp, dexp = expand(ccol, dcol, p)
            w = conv * jax.nn.sigmoid(conv) * dexp
            wb_s[rows, lanes] = w.astype(BF)
            end = cm[:, 5:6] * jnp.exp(cexp[GROUP - 1 :] - cexp)
            wte_s[rows, lanes] = (w * end).astype(BF)
            whole_s[c, 0:1, lanes] = cm[GROUP - 1 :, 4:5] * jnp.exp(cexp[GROUP - 1 :])
        hs_s[c + 1] = whole_s[c, 0:1, :] * hs_s[c] + dot(kt_s[c], wte_s[rows, :])

    g_s[...] = gcar_ref[...].astype(F32)
    dcs[0:8, :] = jnp.zeros((8, CG), F32)
    dcs[count + 8 :, :] = jnp.zeros((8, CG), F32)
    par_ref[:, pl.ds(par_col, CG)] = jnp.zeros((8, CG), F32)

    @pl.loop(0, blocks)
    def _(i):
        c = blocks - 1 - i
        base = pl.multiple_of(c * GROUP, GROUP)
        rows = pl.ds(base, GROUP)
        cm = cm_ref[rows, :]
        bias, scores = bias_s[c], s_s[c]
        dcol, ccol, crow = dcol_ref[0, rows, :], ccol_ref[0, rows, :], crow_ref[0, c]
        gb = g_s[...].astype(BF)
        kg_s[...] = dot(k_s[c], gb)
        hb = hs_s[c].astype(BF)
        qh_s[...] = dot(q_s[c], hb)
        gh = whole_s[c, 0:1, :] * jnp.sum(g_s[...] * hs_s[c], axis=0, keepdims=True)
        lane = lax.broadcasted_iota(jnp.int32, (GROUP, GROUP), 1)
        cols = jnp.zeros((GROUP, GROUP), F32)
        for p in range(HG // 2):
            lanes = slice(p * 128, p * 128 + 128)
            conv = conv_s[rows, lanes]
            sg = jax.nn.sigmoid(conv)
            x = conv * sg
            cum, cexp, dexp = expand(ccol, dcol, p)
            dyb = dy_ref[rows, lanes]
            dy = dyb.astype(F32)
            wb = wb_s[rows, lanes]
            zero = jnp.zeros_like(dyb)
            spread = jnp.concatenate([jnp.where(lo, dyb, zero), jnp.where(lo, zero, dyb)], axis=0)
            dmat = dot(wb, spread, 1, 1)
            decay = [jnp.exp(crow[2 * p + i : 2 * p + i + 1] - cum[i] + bias) for i in range(2)]
            dst_s[c] += dmat[:, :GROUP] * decay[0] + dmat[:, GROUP:] * decay[1]
            mats = [d * scores for d in decay]
            for i in range(2):
                pairs = dmat[:, i * GROUP : (i + 1) * GROUP] * mats[i]
                cols = jnp.where(lane == 2 * p + i, jnp.sum(pairs, axis=1, keepdims=True), cols)
                rr_ref[0, c, 2 * p + i : 2 * p + i + 1, :] = jnp.sum(pairs, axis=0, keepdims=True)
            mats = jnp.concatenate([m.astype(BF) for m in mats], axis=1)
            end = cm[:, 5:6] * jnp.exp(cexp[GROUP - 1 :] - cexp)
            enter = cm[:, 4:5] * jnp.exp(cexp)
            kge = end * kg_s[:, lanes]
            dw = dot(mats, spread) + kge
            edy = enter * dy
            ent_s[:, lanes] = edy.astype(BF)
            kge = wb.astype(F32) * kge
            lt_ref[c, 0:1, pl.ds(par_col + p * 128, 128)] = gh[:, lanes] + jnp.sum(kge, axis=0, keepdims=True)
            skip = tbx_ref[5:6, lanes]
            skx = dy * x
            for n, e in enumerate((edy * qh_s[:, lanes] - kge, x * dw)):
                high = e.astype(BF)
                e_s[0, :, n * CG + p * 128 : n * CG + p * 128 + 128] = high
                e_s[1, :, n * CG + p * 128 : n * CG + p * 128 + 128] = (e - high.astype(F32)).astype(BF)
            dconv = (dexp * dw + skip * dy) * (sg * (1.0 + conv * (1.0 - sg)))
            dcs[pl.ds(base + 8, GROUP), lanes] = dconv
            block = joined[pl.ds(base, GROUP + 8), lanes]
            sums = [
                jnp.sum(dconv * (shifted(block, 5 + k, GROUP) * cm[:, k : k + 1]), axis=0, keepdims=True)
                for k in range(CONV)
            ]
            sums += [jnp.sum(dconv, axis=0, keepdims=True), jnp.sum(skx, axis=0, keepdims=True)]
            par_ref[:, pl.ds(par_col + p * 128, 128)] += jnp.concatenate(sums + [eight[:2]], axis=0)
        entb = ent_s[...]
        dq_s[c] += dot(entb, hb, 1, 1)
        dk_s[c] += dot(wte_s[rows, :], gb, 1, 1)
        g_s[...] = whole_s[c, 0:1, :] * g_s[...] + dot(qt_s[c], entb)
        r_ref[0, rows, :] = dot(e_s[0], one_ref[...]) + dot(e_s[1], one_ref[...]) - cols[:, : 2 * HG]

    def unconv(dcs_ref, tb_ref, width, col):
        for q in range(width // 128):
            lanes = slice(q * 128, q * 128 + 128)
            cols = pl.ds(col + q * 128, 128)

            def pull(start, rows, cm_start):
                block = dcs_ref[pl.ds(start, rows + 8), lanes]
                cm = cm_ref[pl.ds(cm_start, rows + 8), :]
                total = jnp.zeros((rows, 128), F32)
                for k in range(CONV):
                    total = total + tb_ref[k : k + 1, lanes] * shifted(block * cm[:, k : k + 1], 3 - k, rows)
                return total

            @pl.loop(0, blocks)
            def _(c):
                base = pl.multiple_of(c * GROUP, GROUP)
                got = pull(base + 8, GROUP, base)
                px_ref[pl.ds(base, GROUP), cols] = got.astype(BF)
                last_ref[:, cols] = got[GROUP - 8 :]

            block = jnp.concatenate([jnp.zeros((8, 128), F32), dcs_ref[8:16, lanes]], axis=0)
            cm = jnp.concatenate([jnp.zeros((8, 8), F32), cm_ref[0:8, :]], axis=0)
            total = jnp.zeros((8, 128), F32)
            for k in range(CONV):
                total = total + tb_ref[k : k + 1, lanes] * shifted(block * cm[:, k : k + 1], 3 - k, 8)
            gt_ref[:, cols] = total

    unconv(dcs, tbx_ref, CG, par_col)

    @pl.when(step == pl.num_programs(0) - 1)
    def _():
        par_ref[:, INNER:] = jnp.zeros((8, 2 * STATE), F32)

        @pl.loop(0, blocks)
        def _(c):
            base = pl.multiple_of(c * GROUP, GROUP)
            rows = pl.ds(base, GROUP)
            cm = cm_ref[rows, :]
            dst = dst_s[c]
            dk = dk_s[c] + dot(dst.astype(BF), q_s[c])
            dq = dq_s[c] + dot(dst.T.astype(BF), k_s[c])
            for half, grad in enumerate((dk, dq)):
                lanes = slice(half * STATE, half * STATE + STATE)
                conv = kqc_s[rows, lanes]
                sg = jax.nn.sigmoid(conv)
                dconv = grad * (sg * (1.0 + conv * (1.0 - sg)))
                dcs[pl.ds(base + 8, GROUP), lanes] = dconv
                block = joinedkq[pl.ds(base, GROUP + 8), lanes]
                sums = [
                    jnp.sum(dconv * (shifted(block, 5 + k, GROUP) * cm[:, k : k + 1]), axis=0, keepdims=True)
                    for k in range(CONV)
                ]
                sums += [jnp.sum(dconv, axis=0, keepdims=True)]
                par_ref[:, INNER + half * STATE : INNER + half * STATE + STATE] += jnp.concatenate(
                    sums + [eight[:3]], axis=0
                )

        unconv(dcs, tbkq_ref, 2 * STATE, INNER)


def back(xz, xoff, tail, tb, dcol, ccol, crow, cm, srow, dy, incoming, gcar, one):
    count = xz.shape[0]
    blocks = count // GROUP
    steps = HEADS // HG
    vm = pltpu.VMEM
    return pl.pallas_call(
        back_kernel,
        grid=(steps,),
        out_shape=(
            jax.ShapeDtypeStruct((count, XBC), BF),
            jax.ShapeDtypeStruct((steps, count, 2 * HG), F32),
            jax.ShapeDtypeStruct((steps, blocks, HG, GROUP), F32),
            jax.ShapeDtypeStruct((blocks, 8, INNER), F32),
            jax.ShapeDtypeStruct((8, XBC), F32),
            jax.ShapeDtypeStruct((8, XBC), F32),
            jax.ShapeDtypeStruct((8, XBC), F32),
        ),
        in_specs=[
            spec((count, CG), lambda g: (0, xoff // CG + g)),
            spec((count, 2 * STATE), lambda g: (0, (xoff + INNER) // (2 * STATE))),
            spec((8, CG), lambda g: (0, g)),
            spec((8, 2 * STATE), lambda g: (0, INNER // (2 * STATE))),
            spec((8, CG), lambda g: (0, g)),
            spec((8, 2 * STATE), lambda g: (0, INNER // (2 * STATE))),
            spec((1, count, HG), lambda g: (g, 0, 0)),
            spec((1, count, HG), lambda g: (g, 0, 0)),
            spec((1, blocks, HG, GROUP), lambda g: (g, 0, 0, 0)),
            spec((count + 8, 8)),
            spec((blocks, 8, GROUP)),
            spec((count, CG), lambda g: (0, g)),
            spec((STATE, CG), lambda g: (0, g)),
            spec((STATE, CG), lambda g: (0, g)),
            spec((2 * CG, 2 * HG)),
        ],
        out_specs=(
            spec((count, XBC)),
            spec((1, count, 2 * HG), lambda g: (g, 0, 0)),
            spec((1, blocks, HG, GROUP), lambda g: (g, 0, 0, 0)),
            spec((blocks, 8, INNER)),
            spec((8, XBC)),
            spec((8, XBC)),
            spec((8, XBC)),
        ),
        scratch_shapes=[
            vm((count + 8, CG), F32),
            vm((count + 8, 2 * STATE), F32),
            vm((count, 2 * STATE), F32),
            vm((blocks, STATE, GROUP), BF),
            vm((blocks, GROUP, STATE), BF),
            vm((blocks, STATE, GROUP), BF),
            vm((blocks, GROUP, STATE), BF),
            vm((blocks, GROUP, GROUP), F32),
            vm((blocks, GROUP, GROUP), F32),
            vm((count, CG), BF),
            vm((count, CG), BF),
            vm((GROUP, CG), F32),
            vm((GROUP, CG), F32),
            vm((count, CG), F32),
            vm((blocks + 1, STATE, CG), F32),
            vm((STATE, CG), F32),
            vm((blocks, 8, CG), F32),
            vm((GROUP, CG), BF),
            vm((2, GROUP, 2 * CG), BF),
            vm((count + 16, CG), F32),
            vm((blocks, GROUP, GROUP), F32),
            vm((blocks, GROUP, STATE), F32),
            vm((blocks, GROUP, STATE), F32),
        ],
        compiler_params=params(),
        name="mixer_back",
    )(xz, xz, tail, tail, tb, tb, dcol, ccol, crow, cm, srow, dy, incoming, gcar, one)


MESH = pl.DeviceIdType.MESH


class Place:
    def __init__(self, nz):
        dp, self.x = lax.axis_index("dp"), lax.axis_index("seq")
        self.c, self.y, self.z, self.nz = dp % 2, (dp // 2) % 2, dp // 4, nz

    def at(self, z, y, c, x):
        return {"dp": (z * 2 + y) * 2 + c, "seq": x}

    def up(self, r):
        return self.at((self.z + r) % self.nz, self.y, self.c, self.x)

    def flip(self, axis):
        return self.at(
            self.z,
            1 - self.y if axis == "y" else self.y,
            1 - self.c if axis == "c" else self.c,
            1 - self.x if axis == "x" else self.x,
        )

    def greet(self):
        barrier = pltpu.get_barrier_semaphore()
        others = [self.up(r) for r in range(1, self.nz)] + [self.flip(a) for a in "yxc"]
        for other in others:
            pl.semaphore_signal(barrier, inc=1, device_id=other, device_id_type=MESH)
        pl.semaphore_wait(barrier, len(others))


def columns_of(width, tiles):
    total, groups, start = width // 128, [], 0
    while start < total:
        size = min(tiles, total - start)
        if total - start - size == 1:
            size += 1
        groups.append((start * 128, (start + size // 2) * 128, (start + size) * 128))
        start += size
    return groups


def send(src, dst, sems, slot, device):
    copy = pltpu.make_async_remote_copy(
        src_ref=src, dst_ref=dst, send_sem=sems[0].at[slot], recv_sem=sems[1].at[slot],
        device_id=device, device_id_type=MESH,
    )
    copy.start()
    return copy


class Gather:
    def __init__(self, place, ref, cut, sems, first):
        self.p, self.ref, self.cut, self.sems, self.first = place, ref, cut, sems, first
        self.copies = []

    @property
    def slots(self):
        return self.p.nz - 1 + 5

    def push(self, index, slot, device):
        ref = self.ref.at[index]
        copy = send(ref, ref, self.sems, self.first + slot, device)
        self.copies.append(copy)
        return copy

    def phase(self, n):
        p, (a, m, b) = self.p, self.cut
        every, k = slice(None), self.p.nz - 1
        if n == 0:
            self.last = [self.push((p.z, p.y, p.c, p.x, every, slice(a, b)), r - 1, p.up(r)) for r in range(1, p.nz)]
            return
        for copy in self.last:
            copy.wait_recv()
        if n == 1:
            self.last = [
                self.push((every, p.y, p.c, p.x, every, slice(a, m)), k, p.flip("y")),
                self.push((every, p.y, p.c, p.x, every, slice(m, b)), k + 1, p.flip("x")),
            ]
        elif n == 2:
            self.last = [
                self.push((every, every, p.c, p.x, every, slice(a, m)), k + 2, p.flip("x")),
                self.push((every, p.y, p.c, every, every, slice(m, b)), k + 3, p.flip("y")),
            ]
        elif n == 3:
            self.last = [self.push((every, every, p.c, every, every, slice(a, b)), k + 4, p.flip("c"))]

    def drain(self):
        for copy in self.copies:
            copy.wait_send()


def gather_kernel(
    nz, tiles, win_ref, wout_ref, small_ref, hid_ref,
    full_ref, wfull_ref, sfull_ref, normed_ref, proj_ref,
    wbuf, obuf, sbuf, send_sem, recv_sem, own_sem, out_sem,
):
    p = Place(nz)
    own = []
    for i, (src, buf) in enumerate(((small_ref, sbuf), (win_ref, wbuf), (wout_ref, obuf))):
        own.append(pltpu.make_async_copy(src, buf.at[p.z, p.y, p.c, p.x], own_sem.at[i]))
        own[-1].start()
    p.greet()
    jobs = [(sbuf, cut, "small") for cut in columns_of(small_ref.shape[1], small_ref.shape[1] // 128)]
    jobs += [(wbuf, cut, "in") for cut in columns_of(win_ref.shape[1], tiles)]
    jobs += [(obuf, cut, "out") for cut in columns_of(wout_ref.shape[1], tiles // 2 + tiles % 2)]
    per = nz - 1 + 5
    gathers = [Gather(p, buf, cut, (send_sem, recv_sem), per * i) for i, (buf, cut, _) in enumerate(jobs)]
    for copy in own:
        copy.wait()
    outs = []

    def finish(i):
        buf, (a, _, b), kind = jobs[i]
        gathers[i].phase(4)
        if kind == "small":
            gain = jnp.sum(sbuf[...].astype(F32), axis=(0, 1, 2, 3))[0:1]
            rows = hid_ref[...].astype(F32)
            scale = lax.rsqrt(jnp.mean(rows * rows, axis=1, keepdims=True) + norm_eps)
            normed_ref[...] = (rows * scale * gain).astype(BF)
        target = {"small": sfull_ref, "in": full_ref, "out": wfull_ref}[kind]
        every = (slice(None),) * 5
        copy = pltpu.make_async_copy(buf.at[every + (slice(a, b),)], target.at[every + (slice(a, b),)], out_sem.at[i])
        copy.start()
        outs.append(copy)
        if kind == "in":
            weights = buf[:, :, :, :, :, a:b].reshape(-1, b - a)
            proj_ref[:, a:b] = dot(normed_ref[...], weights).astype(BF)

    gathers[0].phase(0)
    for tick in range(len(jobs) + 3):
        if tick + 1 < len(jobs):
            gathers[tick + 1].phase(0)
        for back, n in ((0, 1), (1, 2), (2, 3)):
            if 0 <= tick - back < len(jobs):
                gathers[tick - back].phase(n)
        if tick >= 3:
            finish(tick - 3)
    for g in gathers:
        g.drain()
    for copy in outs:
        copy.wait()


def gather(win, wout, small, hid, nz, tiles=4):
    count, width = hid.shape
    whole = lambda a: jax.ShapeDtypeStruct((nz, 2, 2, 2) + a.shape, BF)
    jobs = 1 + len(columns_of(win.shape[1], tiles)) + len(columns_of(wout.shape[1], tiles // 2 + tiles % 2))
    slots = jobs * (nz - 1 + 5)
    hbm = pl.BlockSpec(memory_space=pl.ANY)
    vmem = pl.BlockSpec(memory_space=pltpu.VMEM)
    dma = pltpu.SemaphoreType.DMA
    full, wfull, sfull, normed, proj = pl.pallas_call(
        functools.partial(gather_kernel, nz, tiles),
        out_shape=(
            whole(win), whole(wout), whole(small),
            jax.ShapeDtypeStruct((count, width), BF),
            jax.ShapeDtypeStruct((count, win.shape[1]), BF),
        ),
        in_specs=[hbm, hbm, hbm, vmem],
        out_specs=(hbm, hbm, hbm, vmem, vmem),
        scratch_shapes=[
            pltpu.VMEM(whole(win).shape, BF), pltpu.VMEM(whole(wout).shape, BF), pltpu.VMEM(whole(small).shape, BF),
            dma((slots,)), dma((slots,)), dma((3,)), dma((jobs,)),
        ],
        compiler_params=params(collective_id=1, has_side_effects=True),
        name="gather_project",
    )(win, wout, small, hid)
    return full, wfull.reshape(-1, wout.shape[1]), sfull, normed, proj


class Scatter:
    def __init__(self, place, part, width, halves, got, sems, first, out):
        self.p, self.part, self.width, self.halves = place, part, width, halves
        self.got, self.sems, self.first, self.out = got, sems, first, out
        self.copies, self.last = [], []

    def push(self, index, dst, slot, device):
        copy = send(self.part.at[index], dst, self.sems, self.first + slot, device)
        self.copies.append(copy)
        self.last.append(copy)

    def add(self, index, got):
        self.part[index] = (self.part[index].astype(F32) + got.astype(F32)).astype(self.part.dtype)

    def phase(self, n):
        p, every, k = self.p, slice(None), self.p.nz - 1
        z, y, c, x = p.z, p.y, p.c, p.x
        cols = slice(0, self.width)
        for copy in self.last:
            copy.wait_recv()
        self.last = []
        core, first, second, ring = self.got
        if n == 0:
            self.push((every, every, 1 - c, every, every, cols), core.at[..., cols], k + 4, p.flip("c"))
        elif n == 1:
            for i in range(p.nz):
                self.add((i, every, c, every, every, cols), core[i, :, :, :, cols])
            for i, (axis, lo, hi) in enumerate(self.halves):
                index = (every, every, c, 1 - x) if axis == "x" else (every, 1 - y, c, every)
                self.push(index + (every, slice(lo, hi)), first.at[i, :, :, :, 0 : hi - lo], k + i, p.flip(axis))
        elif n == 2:
            for i, (axis, lo, hi) in enumerate(self.halves):
                index = (every, every, c, x) if axis == "x" else (every, y, c, every)
                self.add(index + (every, slice(lo, hi)), first[i, :, :, :, 0 : hi - lo])
                index = (every, 1 - y, c, x) if axis == "x" else (every, y, c, 1 - x)
                other = p.flip("y" if axis == "x" else "x")
                self.push(index + (every, slice(lo, hi)), second.at[i, :, :, 0 : hi - lo], k + 2 + i, other)
        elif n == 3:
            for i, (axis, lo, hi) in enumerate(self.halves):
                self.add((every, y, c, x, every, slice(lo, hi)), second[i, :, :, 0 : hi - lo])
            for r in range(1, p.nz):
                index = (lax.rem(z + r, p.nz), y, c, x, every, cols)
                self.push(index, ring.at[r - 1, :, cols], r - 1, p.up(r))
        else:
            total = self.part[z, y, c, x, :, cols].astype(F32)
            for r in range(p.nz - 1):
                total = total + ring[r, :, cols].astype(F32)
            self.out(total)
            for copy in self.copies:
                copy.wait_send()


RING = 5


def scatter_kernel(
    nz, tiles,
    nt_ref, it_ref, cot_ref, pz_ref, px_ref, pd_ref, full_ref, hid_ref, gain_ref, small_ref,
    gin_ref, gout_ref, gsmall_ref, ng_ref,
    part_big, part_small, core_big, core_small, first_big, first_small, second_big, second_small,
    ring_big, ring_small, wbuf, gbuf, send_sem, recv_sem, w_sem, g_sem,
):
    p = Place(nz)
    per = nz - 1 + 5
    cuts = columns_of(full_ref.shape[5], tiles)
    splits = it_ref.shape[1]
    jobs = [("out", cut, r) for r in range(splits) for cut in columns_of(cot_ref.shape[1], tiles)]
    jobs += [("in", cut, 0) for cut in cuts]
    jobs += [("small", (0, 128, 128), 0)]
    n_in = len(cuts)
    deep = nt_ref.shape[0] // (8 * nz)
    every = (slice(None),) * 5

    class Fetch:
        def __init__(self, i):
            a, _, b = cuts[i]
            self.copies = [
                pltpu.make_async_copy(
                    full_ref.at[every + (slice(a, b),)], wbuf.at[i % 2, :, :, :, :, :, 0 : b - a], w_sem.at[i % 2]
                )
            ]
            start = 0
            for n, ref in enumerate((pz_ref, px_ref, pd_ref)):
                lo, hi = max(a, start), min(b, start + ref.shape[1])
                if lo < hi:
                    self.copies.append(
                        pltpu.make_async_copy(
                            ref.at[:, lo - start : hi - start], gbuf.at[i % 2, :, lo - a : hi - a], g_sem.at[i % 2, n]
                        )
                    )
                start += ref.shape[1]

        def start(self):
            for copy in self.copies:
                copy.start()

        def wait(self):
            for copy in self.copies:
                copy.wait()

    fetches = [Fetch(i) for i in range(n_in)]
    fetches[0].start()
    p.greet()
    scatters = []
    for i, (kind, (a, m, b), r) in enumerate(jobs):
        if kind == "small":
            part, got, n = part_small, (core_small, first_small, second_small, ring_small), 0
        else:
            part, got, n = part_big.at[i % RING], (core_big, first_big, second_big, ring_big), i
        halves = [("x", 0, m - a)] + ([("y", m - a, b - a)] if b > m else [])

        def out(total, kind=kind, a=a, b=b, r=r):
            ref = {"in": gin_ref, "out": gout_ref, "small": gsmall_ref}[kind]
            ref[r * deep : r * deep + total.shape[0], a:b] = total

        scatters.append(
            Scatter(
                p, part, b - a, halves, [g.at[n] for g in got], (send_sem, recv_sem), per * i, out
            )
        )

    done = {"in": 0}

    def fill(i):
        kind, (a, _, b), r = jobs[i]
        if kind == "small":
            rows = hid_ref[...].astype(F32)
            scale = lax.rsqrt(jnp.mean(rows * rows, axis=1, keepdims=True) + norm_eps)
            unit = rows * scale
            grad = ng_ref[...]
            gpre = jnp.sum(grad * unit, axis=0, keepdims=True)
            grad = grad * gain_ref[0:1, :]
            grad = scale * (grad - unit * jnp.mean(grad * unit, axis=1, keepdims=True))
            ng_ref[...] = cot_ref[...].astype(F32) + grad
            gpre = jnp.broadcast_to(gpre, (8, gpre.shape[1]))
            share = gpre.shape[1] // (8 * nz)
            part_small[...] = small_ref[...]
            for j in range(8 * nz):
                moved = gpre if j == 0 else pltpu.roll(gpre, gpre.shape[1] - share * j, 1)
                part_small[j // 8, j // 4 % 2, j // 2 % 2, j % 2, 7:8, :] = moved[0:1, :128]
            return
        part = scatters[i].part
        high = deep * 8
        if kind == "out":
            right = cot_ref[:, a:b]
        else:
            n = done["in"]
            done["in"] += 1
            fetches[n].wait()
            if n + 1 < n_in:
                fetches[n + 1].start()
            right = gbuf[n % 2, :, 0 : b - a]
        for k in range(nz):
            if kind == "out":
                left = it_ref[k * 8 : k * 8 + 8, r].reshape(high, -1)
            else:
                left = nt_ref[k * high : (k + 1) * high, :]
            block = dot(left, right).astype(BF)
            part[k, :, :, :, :, 0 : b - a] = block.reshape(2, 2, 2, deep, b - a)

    def pull(i):
        kind, (a, _, b), _ = jobs[i]
        if kind == "in":
            n = done["in"] - 1
            weights = wbuf[n % 2, :, :, :, :, :, 0 : b - a].reshape(-1, b - a)
            grown = dot(gbuf[n % 2, :, 0 : b - a], weights, 1, 1)
            if n == 0:
                ng_ref[...] = grown
            else:
                ng_ref[...] += grown

    for tick in range(len(jobs) + 4):
        for back in (4, 3, 2, 1):
            if 0 <= tick - back < len(jobs):
                scatters[tick - back].phase(back)
        if tick < len(jobs):
            fill(tick)
            scatters[tick].phase(0)
            pull(tick)


def scatter(normed_t, inner_t, cot, pz, px, pd, full, hid, gain, small, nz, tiles=4):
    rows_in, rows_out = normed_t.shape[0] // (8 * nz), inner_t.shape[0] // (8 * nz)
    width_in, width_out = pz.shape[1] + px.shape[1] + pd.shape[1], cot.shape[1]
    splits = rows_out // rows_in
    n_in, n_out = len(columns_of(width_in, tiles)), splits * len(columns_of(width_out, tiles))
    inner_t = inner_t.reshape(8 * nz, splits, rows_in, inner_t.shape[1])
    hbm = pl.BlockSpec(memory_space=pl.ANY)
    vmem = pl.BlockSpec(memory_space=pltpu.VMEM)
    dma = pltpu.SemaphoreType.DMA
    vm = pltpu.VMEM
    w = tiles * 128
    shapes = [(n_in + n_out, rows_in, w, BF), (1, 8, 128, F32)]
    parts = [vm((RING, nz, 2, 2, 2, rows_in, w), BF), vm((nz, 2, 2, 2, 8, 128), F32)]
    core = [vm((n, nz, 2, 2, r, w), t) for n, r, w, t in shapes]
    first = [vm((n, 2, nz, 2, r, max(w // 2, 128)), t) for n, r, w, t in shapes]
    second = [vm((n, 2, nz, r, max(w // 2, 128)), t) for n, r, w, t in shapes]
    ring = [vm((n, nz - 1, r, w), t) for n, r, w, t in shapes]
    slots = (n_in + n_out + 1) * (nz - 1 + 5)
    return pl.pallas_call(
        functools.partial(scatter_kernel, nz, tiles),
        out_shape=(
            jax.ShapeDtypeStruct((rows_in, width_in), F32),
            jax.ShapeDtypeStruct((rows_out, width_out), F32),
            jax.ShapeDtypeStruct((8, 128), F32),
            jax.ShapeDtypeStruct(hid.shape, F32),
        ),
        in_specs=[vmem] * 3 + [hbm] * 4 + [vmem] * 3,
        out_specs=(vmem,) * 4,
        scratch_shapes=parts + core + first + second + ring + [
            vm((2, nz, 2, 2, 2, rows_in, w), BF), vm((2, cot.shape[0], w), BF),
            dma((slots,)), dma((slots,)), dma((2,)), dma((2, 3)),
        ],
        compiler_params=pltpu.CompilerParams(
            vmem_limit_bytes=67043328, collective_id=2, has_side_effects=True
        ),
        name="grads_scatter",
    )(normed_t, inner_t, cot, pz, px, pd, full, hid, gain, small)


def passed_along(shard, axis, by):
    count = lax.axis_size(axis)
    pairs = [(i, i + by) for i in range(count) if 0 <= i + by < count]
    return lax.ppermute(shard, axis, pairs)


def chained(own, factor, axis, by):
    got = jnp.zeros(own.shape, BF)
    for i in range(lax.axis_size(axis) - 1):
        sent = own if i == 0 else own.astype(F32) + factor * got.astype(F32)
        got = passed_along(sent.astype(BF), axis, by)
    return got


def adamw(weight, grad, mean, square, rate, decay):
    new_mean = first_beta * mean + (1.0 - first_beta) * grad
    new_square = second_beta * square + (1.0 - second_beta) * grad * grad
    corrected = new_mean / (1.0 - first_beta**STEP)
    spread = jnp.sqrt(new_square / (1.0 - second_beta**STEP))
    new_weight = weight * (1.0 - rate * decay) - rate * corrected / (spread + adam_eps)
    return (new_weight, new_mean, new_square)


def prepare(step_raw, seg_ext, step_bias, decay_log):
    count = step_raw.shape[0]
    blocks, steps = count // GROUP, HEADS // HG
    delta = jax.nn.softplus(step_raw + step_bias[None, :])
    logdec = -delta * jnp.exp(decay_log)[None, :]
    lower = jnp.tril(jnp.ones((GROUP, GROUP), F32))
    cum = jnp.einsum("ij,cjh->cih", lower, logdec.reshape(blocks, GROUP, HEADS), precision=HIGHEST)
    own = seg_ext[CONV - 1 :]
    seg_blocks = own.reshape(blocks, GROUP)
    before = jnp.concatenate([seg_ext[CONV - 2 : CONV - 1], seg_blocks[:-1, -1]])
    columns = [seg_ext[k : k + count] == own for k in range(CONV)]
    columns += [(seg_blocks == before[:, None]).reshape(count), (seg_blocks == seg_blocks[:, -1:]).reshape(count)]
    columns = [c.astype(F32) for c in columns] + [own.astype(F32), jnp.zeros((count,), F32)]
    cm = jnp.pad(jnp.stack(columns, axis=1), ((0, 8), (0, 0)))
    srow = jnp.broadcast_to(seg_blocks.astype(F32)[:, None, :], (blocks, 8, GROUP))
    dcol = delta.reshape(count, steps, HG).transpose(1, 0, 2)
    ccol = cum.reshape(count, steps, HG).transpose(1, 0, 2)
    crow = cum.reshape(blocks, GROUP, steps, HG).transpose(2, 0, 3, 1)
    return delta, logdec, (dcol, ccol, crow, cm, srow)


def shards(
    hidden,
    cotangent,
    segments,
    weight_in,
    weight_out,
    gain_pre,
    gain_gated,
    conv_taps,
    conv_bias,
    decay_log,
    skip_gain,
    step_bias,
    mean_weight_in,
    square_weight_in,
    mean_weight_out,
    square_weight_out,
    mean_gain_pre,
    square_gain_pre,
    mean_gain_gated,
    square_gain_gated,
    mean_conv_taps,
    square_conv_taps,
    mean_conv_bias,
    square_conv_bias,
    mean_decay_log,
    square_decay_log,
    mean_skip_gain,
    square_skip_gain,
    mean_step_bias,
    square_step_bias,
):
    piece = hidden.shape[1]
    blocks, steps = piece // GROUP, HEADS // HG
    devices = lax.axis_size("dp") * lax.axis_size("seq")
    offset = lax.axis_index("seq") * piece
    lead = jnp.full((CONV - 1,), -1, jnp.int32)
    seg_ext = lax.dynamic_slice_in_dim(jnp.concatenate([lead, segments[0]]), offset, piece + CONV - 1)

    sizes = (gain_pre.shape[0], gain_gated.shape[0], conv_taps.size, conv_bias.shape[0])
    small = jnp.concatenate([gain_pre, gain_gated, conv_taps.reshape(-1), conv_bias]).astype(BF)
    me = lax.axis_index("dp") * lax.axis_size("seq") + lax.axis_index("seq")
    width = hidden.shape[2]
    padded = -(-weight_in.shape[1] // 128) * 128
    win_low = jnp.pad(weight_in.astype(BF), ((0, 0), (0, padded - weight_in.shape[1])))
    rows = hidden[0].astype(F32)
    scale = lax.rsqrt(jnp.mean(rows * rows, axis=-1, keepdims=True) + norm_eps)
    nz = lax.axis_size("dp") // 4
    own = weight_in.shape[0] % 16 == 0 and lax.axis_size("seq") == 2 and lax.axis_size("dp") == 4 * nz
    if own:
        placed = lax.dynamic_update_slice_in_dim(jnp.zeros((width,), BF), gain_pre.astype(BF), me * sizes[0], 0)
        block = jnp.stack([placed, jnp.pad(small, (0, width - small.shape[0]))])
        block = jnp.pad(block, ((0, 6), (0, 0)))
        full, w_out, small, normed, proj = gather(win_low, weight_out.astype(BF), block, hidden[0], nz)
        small = small.reshape(devices, 8, width)[:, 1, : sum(sizes)].astype(F32)
    else:
        small = lax.all_gather(small, BOTH, axis=0).astype(F32)
        w_in = lax.all_gather(win_low, BOTH, axis=0, tiled=True)
        w_out = lax.all_gather(weight_out.astype(BF), BOTH, axis=0, tiled=True)
    cuts = [0]
    for s in sizes:
        cuts.append(cuts[-1] + s)
    pre_gain, gated_gain, taps, cbias = [small[:, a:b] for a, b in zip(cuts, cuts[1:])]
    pre_gain, gated_gain, cbias = pre_gain.reshape(-1), gated_gain.reshape(-1), cbias.reshape(-1)
    taps = taps.reshape(devices, CONV, -1).transpose(1, 0, 2).reshape(CONV, XBC)

    if not own:
        normed = (rows * scale * pre_gain).astype(BF)
        proj = jnp.dot(normed, w_in, preferred_element_type=F32).astype(BF)
    tail = passed_along(proj[piece - CONV + 1 :, INNER : INNER + XBC], "seq", 1)
    tail = jnp.pad(tail, ((8 - CONV + 1, 0), (0, 0)))
    skip_lanes = jnp.pad(jnp.repeat(skip_gain, HEAD_DIM), (0, XBC - INNER))
    tb = jnp.concatenate([taps, cbias[None], skip_lanes[None], jnp.zeros((2, XBC), F32)])
    step_raw = proj[:, INNER + XBC : INNER + XBC + HEADS].astype(F32)
    delta, logdec, prepared = prepare(step_raw, seg_ext, step_bias, decay_log)

    mixed, reach, queries, carried, passed = front(proj, INNER, tail, tb, *prepared)
    incoming = chained(carried, passed[:1], "seq", 1)
    gain8 = jnp.broadcast_to(gated_gain[None], (8, INNER))
    output, inner, dy, dz, ginc, ggain = middle(
        mixed, reach, queries, incoming, proj, hidden[0], cotangent[0], gain8, w_out
    )
    grad_gated = ggain[0]
    gcar = chained(ginc, passed[:1], "seq", -1)
    group = jnp.arange(2 * CG) // HEAD_DIM
    two = (group[:, None] == jnp.arange(2 * HG)[None, :]).astype(BF)
    px, r, rr, lt, par, gt, last = back(proj, INNER, tail, tb, *prepared, dy, incoming, gcar, two)
    returned = passed_along(gt[8 - CONV + 1 :].astype(BF), "seq", -1).astype(F32)
    patched = (last[8 - CONV + 1 :] + returned).astype(BF)
    px = px.at[piece - CONV + 1 :].set(patched)

    r = r.transpose(1, 0, 2)
    r1, r2 = r[..., :HG].reshape(piece, HEADS), r[..., HG:].reshape(piece, HEADS)
    dcum = r1.reshape(blocks, GROUP, HEADS) + rr.transpose(1, 3, 0, 2).reshape(blocks, GROUP, HEADS)
    ends = jnp.sum(lt[:, 0].reshape(blocks, HEADS, HEAD_DIM), axis=-1)
    upper = jnp.triu(jnp.ones((GROUP, GROUP), F32))
    dlogdec = jnp.einsum("ij,cjh->cih", upper, dcum, precision=HIGHEST) + ends[:, None, :]
    dlogdec = dlogdec.reshape(piece, HEADS)
    dstep = (r2 - jnp.exp(decay_log)[None] * dlogdec) * jax.nn.sigmoid(step_raw + step_bias[None])
    grad_dlog = jnp.sum(dlogdec * logdec, axis=0)
    grad_sbias = jnp.sum(dstep, axis=0)
    grad_skip = jnp.sum(par[5, :INNER].reshape(HEADS, HEAD_DIM), axis=-1)
    grad_taps, grad_cbias = par[:CONV], par[4]

    pd = jnp.pad(dstep.astype(BF), ((0, 0), (0, padded - INNER - XBC - HEADS)))
    heads = jnp.concatenate([grad_dlog, grad_skip, grad_sbias])
    count_in = weight_in.shape[1]
    if own:
        smalls = [
            grad_gated.reshape(devices, -1),
            grad_taps.reshape(CONV, devices, -1).transpose(1, 0, 2).reshape(devices, -1),
            grad_cbias.reshape(devices, -1),
            jnp.broadcast_to(heads[None], (devices, heads.shape[0])),
        ]
        smalls = jnp.concatenate(smalls, axis=1)
        smalls = jnp.pad(smalls, ((0, 0), (0, 1024 - smalls.shape[1]))).reshape(nz, 2, 2, 2, 8, 128)
        gain_row = jnp.broadcast_to(pre_gain[None], (8, width))
        share_in, share_out, share, input_grad = scatter(
            normed.T, inner.T, cotangent[0], dz, px, pd, full, hidden[0], gain_row, smalls, nz
        )
        share_in = share_in[:, :count_in]
        flat = share.reshape(-1)
        cuts = [0]
        for s in sizes[1:] + (heads.shape[0],):
            cuts.append(cuts[-1] + s)
        own_gated, own_taps, own_cbias, heads = [flat[a:b] for a, b in zip(cuts, cuts[1:])]
        own_pre, own_taps = share[7, : sizes[0]], own_taps.reshape(CONV, -1)
    else:
        proj_grad = jnp.concatenate([dz, px, pd], axis=1)
        grad_wout = jnp.dot(inner.T, cotangent[0], preferred_element_type=F32)
        grad_win = jnp.dot(normed.T, proj_grad[:, :count_in], preferred_element_type=F32)
        normed_grad = jnp.dot(proj_grad, w_in.T, preferred_element_type=F32)
        unit = rows * scale
        grad_pre = jnp.sum(normed_grad * unit, axis=0)
        pulled = normed_grad * pre_gain
        pulled = scale * (pulled - unit * jnp.mean(pulled * unit, axis=-1, keepdims=True))
        input_grad = cotangent[0].astype(F32) + pulled

        def scattered(total):
            return lax.psum_scatter(total.astype(BF), BOTH, scatter_dimension=0, tiled=True).astype(F32)

        share_in, share_out = scattered(grad_win), scattered(grad_wout)
        smalls = (grad_pre, grad_gated, grad_taps.reshape(-1), grad_cbias, heads)
        summed = lax.psum(jnp.concatenate(smalls), BOTH)
        pieces, start = [], 0
        for s in smalls:
            pieces.append(summed[start : start + s.shape[0]])
            start += s.shape[0]
        own_pre, own_gated = [lax.dynamic_slice_in_dim(pieces[n], me * sizes[n], sizes[n]) for n in range(2)]
        own_taps = lax.dynamic_slice_in_dim(
            pieces[2].reshape(CONV, XBC), me * conv_taps.shape[1], conv_taps.shape[1], axis=1
        )
        own_cbias = lax.dynamic_slice_in_dim(pieces[3], me * sizes[3], sizes[3])
        heads = pieces[4]
    sum_dlog, sum_skip, sum_sbias = [heads[n * HEADS : (n + 1) * HEADS] for n in range(3)]
    grads = (share_in, share_out, own_pre, own_gated, own_taps, own_cbias, sum_dlog, sum_skip, sum_sbias)
    weights = (
        weight_in,
        weight_out,
        gain_pre,
        gain_gated,
        conv_taps,
        conv_bias,
        decay_log,
        skip_gain,
        step_bias,
    )
    means = (
        mean_weight_in,
        mean_weight_out,
        mean_gain_pre,
        mean_gain_gated,
        mean_conv_taps,
        mean_conv_bias,
        mean_decay_log,
        mean_skip_gain,
        mean_step_bias,
    )
    squares = (
        square_weight_in,
        square_weight_out,
        square_gain_pre,
        square_gain_gated,
        square_conv_taps,
        square_conv_bias,
        square_decay_log,
        square_skip_gain,
        square_step_bias,
    )
    rates = (0.01, 0.01, 0.1, 0.1, 0.1, 0.1, 0.1, 0.1, 0.1)
    decays = (0.1, 0.1, 0.0, 0.0, 0.0, 0.0, 0.0, 0.0, 0.0)
    updated = [
        adamw(weights[index], grads[index], means[index], squares[index], rates[index], decays[index])
        for index in range(9)
    ]
    new_weights = tuple((entry[0] for entry in updated))
    new_means = tuple((entry[1] for entry in updated))
    new_squares = tuple((entry[2] for entry in updated))
    return (output[None], input_grad[None]) + grads + new_weights + new_means + new_squares


def solution(mesh):
    dp, seq, both = P("dp"), P("seq"), P(BOTH)
    rows, cols, copied = P(BOTH, None), P(None, BOTH), P()
    whole = P("dp", "seq", None)
    kinds = (rows, rows, both, both, cols, both, copied, copied, copied)
    pairs = tuple(kind for kind in kinds for _ in range(2))
    return jax.shard_map(
        shards,
        mesh=mesh,
        in_specs=(whole, whole, P("dp", None)) + kinds + pairs,
        out_specs=(whole, whole) + kinds * 4,
        check_vma=False,
    )
```

```python
import functools

import jax
import jax.numpy as jnp
from jax import lax
from jax.experimental import pallas as pl
from jax.experimental.pallas import tpu as pltpu
from jax.sharding import PartitionSpec as P

INNER = 3072
HEADS = 48
HEAD_DIM = 64
STATE = 128
CONV = 4
GROUP = 128
STEP = 4
XBC = 3328

norm_eps = 1e-05
first_beta = 0.9
second_beta = 0.999
adam_eps = 1e-08
HIGHEST = lax.Precision.HIGHEST
BOTH = ("dp", "seq")

HG = 8
CG = HG * HEAD_DIM
F32 = jnp.float32
BF = jnp.bfloat16
NEG = -1e30


def dot(a, b, ca=1, cb=0, precision=None):
    return lax.dot_general(
        a, b, (((ca,), (cb,)), ((), ())), precision=precision, preferred_element_type=F32
    )


def low_lanes(rows):
    return lax.broadcasted_iota(jnp.int32, (rows, 2 * HEAD_DIM), 1) < HEAD_DIM


def shifted(block, by, rows):
    if by % 8 == 0:
        return block[by : by + rows]
    return pltpu.roll(block, block.shape[0] - by, 0)[:rows]


def conv_block(joined, base, lanes, tb_ref, cm):
    block = joined[pl.ds(base, GROUP + 8), lanes]
    total = tb_ref[4:5, lanes] + jnp.zeros((GROUP, 1), F32)
    for k in range(CONV):
        total = total + tb_ref[k : k + 1, lanes] * (shifted(block, 5 + k, GROUP) * cm[:, k : k + 1])
    return total


def fill_joined(joined, tail_ref, x_ref):
    joined[0:8, :] = tail_ref[...].astype(F32)
    joined[8:, :] = x_ref[...].astype(F32)


def bias_of(cm_ref, srow_ref, c, base, turned):
    seg_col = cm_ref[pl.ds(base, GROUP), 6:7]
    seg_row = srow_ref[c, 0:1, :]
    down = lax.broadcasted_iota(jnp.int32, (GROUP, GROUP), 0)
    across = lax.broadcasted_iota(jnp.int32, (GROUP, GROUP), 1)
    order = (across >= down) if turned else (down >= across)
    return jnp.where(order & (seg_col == seg_row), 0.0, NEG)


def greet_across():
    barrier = pltpu.get_barrier_semaphore()
    pl.semaphore_signal(barrier, inc=1, device_id=other_piece(), device_id_type=pl.DeviceIdType.MESH)
    pl.semaphore_wait(barrier, 1)


def other_piece():
    return {"dp": lax.axis_index("dp"), "seq": 1 - lax.axis_index("seq")}


def across(src, dst, sems, slot):
    return pltpu.make_async_remote_copy(
        src_ref=src, dst_ref=dst, send_sem=sems.at[0, slot], recv_sem=sems.at[1, slot],
        device_id=other_piece(), device_id_type=pl.DeviceIdType.MESH,
    )


def front_kernel(
    remote, x_ref, kq_ref, tailx_ref, tailkq_ref, tbx_ref, tbkq_ref, dcol_ref, ccol_ref, crow_ref, cm_ref, srow_ref,
    y_ref, reach_ref, q_ref, car_ref, pas_ref,
    joined, joinedkq, kt_s, q_s, s_s, bias_s, wte_s, inter_s, state_s, fac_s, whole_s, car_s, sems,
):
    count = x_ref.shape[0]
    blocks = count // GROUP
    lo = low_lanes(GROUP)
    step = pl.program_id(0)

    @pl.when(step == 0)
    def _():
        if remote:
            greet_across()
        fill_joined(joinedkq, tailkq_ref, kq_ref)

        @pl.loop(0, blocks)
        def _(c):
            base = pl.multiple_of(c * GROUP, GROUP)
            cm = cm_ref[pl.ds(base, GROUP), :]
            parts = []
            for half in range(2):
                conv = conv_block(joinedkq, base, slice(half * STATE, half * STATE + STATE), tbkq_ref, cm)
                parts.append(conv * jax.nn.sigmoid(conv))
            keys, queries = parts
            kt_s[c] = keys.T.astype(BF)
            q_s[c] = queries.astype(BF)
            q_ref[pl.ds(base, GROUP), :] = queries.astype(BF)
            s_s[c] = dot(queries, keys, 1, 1, HIGHEST)
            bias_s[c] = bias_of(cm_ref, srow_ref, c, base, False)

    fill_joined(joined, tailx_ref, x_ref)
    state_s[...] = jnp.zeros_like(state_s)
    fac_s[...] = jnp.ones_like(fac_s)

    @pl.loop(0, blocks)
    def _(c):
        base = pl.multiple_of(c * GROUP, GROUP)
        rows = pl.ds(base, GROUP)
        cm = cm_ref[rows, :]
        enter_mask, end_mask = cm[:, 4:5], cm[:, 5:6]
        bias, scores = bias_s[c], s_s[c]
        dcol, ccol, crow = dcol_ref[0, rows, :], ccol_ref[0, rows, :], crow_ref[0, c]
        inter_s[...] = dot(q_s[c], state_s[...].astype(BF))
        for p in range(HG // 2):
            lanes = slice(p * 128, p * 128 + 128)
            conv = conv_block(joined, base, lanes, tbx_ref, cm)
            x = conv * jax.nn.sigmoid(conv)
            cum = [jnp.broadcast_to(ccol[:, h : h + 1], (GROUP, GROUP)) for h in (2 * p, 2 * p + 1)]
            cexp = jnp.where(lo, cum[0], cum[1])
            dexp = jnp.where(lo, dcol[:, 2 * p : 2 * p + 1], dcol[:, 2 * p + 1 : 2 * p + 2])
            w = x * dexp
            wb = w.astype(BF)
            enter = enter_mask * jnp.exp(cexp)
            wte_s[:, lanes] = (w * (end_mask * jnp.exp(cexp[GROUP - 1 :] - cexp))).astype(BF)
            mats = [
                (jnp.exp(cum[i] - crow[2 * p + i : 2 * p + i + 1] + bias) * scores).astype(BF)
                for i in range(2)
            ]
            zero = jnp.zeros_like(wb)
            spread = jnp.concatenate([jnp.where(lo, wb, zero), jnp.where(lo, zero, wb)], axis=0)
            y = dot(jnp.concatenate(mats, axis=1), spread)
            y_ref[rows, lanes] = y + enter * inter_s[:, lanes] + tbx_ref[5:6, lanes] * x
            reach_ref[rows, lanes] = (enter * fac_s[0:1, lanes]).astype(BF)
            whole_s[0:1, lanes] = enter[GROUP - 1 :]
        state_s[...] = whole_s[0:1, :] * state_s[...] + dot(kt_s[c], wte_s[...])
        fac_s[0:1, :] = fac_s[0:1, :] * whole_s[0:1, :]

    pas_ref[...] = fac_s[...]
    if not remote:
        car_ref[...] = state_s[...].astype(BF)
        return

    def moved(g):
        cols = pl.ds(pl.multiple_of(g * CG, CG), CG)
        return across(car_s.at[g], car_ref.at[:, cols], sems, g)

    car_s[step] = state_s[...].astype(BF)
    moved(step).start()

    @pl.when(step == pl.num_programs(0) - 1)
    def _():
        for g in range(HEADS // HG):
            moved(g).wait()


def spec(shape, index=None, **kw):
    if index is None:
        index = lambda *_: (0,) * len(shape)
    return pl.BlockSpec(shape, index, **kw)


def params(**kw):
    return pltpu.CompilerParams(vmem_limit_bytes=60 << 20, **kw)


def front(xz, xoff, tail, tb, dcol, ccol, crow, cm, srow, remote):
    count = xz.shape[0]
    blocks = count // GROUP
    steps = HEADS // HG
    vm = pltpu.VMEM
    return pl.pallas_call(
        functools.partial(front_kernel, remote),
        grid=(steps,),
        out_shape=(
            jax.ShapeDtypeStruct((count, INNER), F32),
            jax.ShapeDtypeStruct((count, INNER), BF),
            jax.ShapeDtypeStruct((count, STATE), BF),
            jax.ShapeDtypeStruct((STATE, INNER), BF),
            jax.ShapeDtypeStruct((8, INNER), F32),
        ),
        in_specs=[
            spec((count, CG), lambda g: (0, xoff // CG + g)),
            spec((count, 2 * STATE), lambda g: (0, (xoff + INNER) // (2 * STATE))),
            spec((8, CG), lambda g: (0, g)),
            spec((8, 2 * STATE), lambda g: (0, INNER // (2 * STATE))),
            spec((8, CG), lambda g: (0, g)),
            spec((8, 2 * STATE), lambda g: (0, INNER // (2 * STATE))),
            spec((1, count, HG), lambda g: (g, 0, 0)),
            spec((1, count, HG), lambda g: (g, 0, 0)),
            spec((1, blocks, HG, GROUP), lambda g: (g, 0, 0, 0)),
            spec((count + 8, 8)),
            spec((blocks, 8, GROUP)),
        ],
        out_specs=(
            spec((count, CG), lambda g: (0, g)),
            spec((count, CG), lambda g: (0, g)),
            spec((count, STATE)),
            pl.BlockSpec(memory_space=pl.ANY) if remote else spec((STATE, CG), lambda g: (0, g)),
            spec((8, CG), lambda g: (0, g)),
        ),
        scratch_shapes=[
            vm((count + 8, CG), F32),
            vm((count + 8, 2 * STATE), F32),
            vm((blocks, STATE, GROUP), BF),
            vm((blocks, GROUP, STATE), BF),
            vm((blocks, GROUP, GROUP), F32),
            vm((blocks, GROUP, GROUP), F32),
            vm((GROUP, CG), BF),
            vm((GROUP, CG), F32),
            vm((STATE, CG), F32),
            vm((8, CG), F32),
            vm((8, CG), F32),
            vm((steps, STATE, CG), BF),
            pltpu.SemaphoreType.DMA((2, steps)),
        ],
        compiler_params=params(**(dict(collective_id=3, has_side_effects=True) if remote else {})),
        name="mixer_front",
    )(xz, xz, tail, tail, tb, tb, dcol, ccol, crow, cm, srow)


def middle_kernel(
    y_ref, reach_ref, q_ref, inc_ref, z_ref, hid_ref, cot_ref, gain_ref, wout_ref, flag_ref,
    out_ref, it_ref, dy_ref, dz_ref, ginc_ref, ggain_ref, sum_s,
):
    @pl.when(pl.program_id(0) == 0)
    def _():
        sum_s[...] = jnp.zeros_like(sum_s)
        ggain_ref[...] = jnp.zeros_like(ggain_ref)

    gain = gain_ref[0:1, :]
    reach = reach_ref[...].astype(F32) * flag_ref[0:1, 0:1]
    full = y_ref[...] + reach * dot(q_ref[...], inc_ref[...])
    z = z_ref[...].astype(F32)
    sg = jax.nn.sigmoid(z)
    gated = full * (z * sg)
    scale = lax.rsqrt(jnp.mean(gated * gated, axis=1, keepdims=True) + norm_eps)
    unit = gated * scale
    inner = (unit * gain).astype(BF)
    it_ref[...] = inner.T
    out_ref[...] = (hid_ref[...].astype(F32) + dot(inner, wout_ref[...])).astype(BF)
    grad = dot(cot_ref[...], wout_ref[...], 1, 1)
    ggain_ref[0:1, :] += jnp.sum(grad * unit, axis=0, keepdims=True)
    grad = grad * gain
    grad = scale * (grad - unit * jnp.mean(grad * unit, axis=1, keepdims=True))
    dz_ref[...] = (grad * full * (sg * (1.0 + z * (1.0 - sg)))).astype(BF)
    dyb = (grad * (z * sg)).astype(BF)
    dy_ref[...] = dyb
    dy = dyb.astype(F32)
    sum_s[...] += dot(q_ref[...].astype(F32).T.astype(BF), (dy * reach).astype(BF))

    @pl.when(pl.program_id(0) == pl.num_programs(0) - 1)
    def _():
        ginc_ref[...] = sum_s[...].astype(BF)


def middle(y, reach, q, incoming, proj, hid, cot, gain, wout, flag):
    count, width = hid.shape
    blocks = count // GROUP
    row = lambda w: spec((GROUP, w), lambda c: (c, 0))
    once = dict(pipeline_mode=pl.Buffered(1))
    return pl.pallas_call(
        middle_kernel,
        grid=(blocks,),
        out_shape=(
            jax.ShapeDtypeStruct((count, width), BF),
            jax.ShapeDtypeStruct((INNER, count), BF),
            jax.ShapeDtypeStruct((count, INNER), BF),
            jax.ShapeDtypeStruct((count, INNER), BF),
            jax.ShapeDtypeStruct((STATE, INNER), BF),
            jax.ShapeDtypeStruct((8, INNER), F32),
        ),
        in_specs=[
            row(INNER), row(INNER), row(STATE), spec((STATE, INNER)), row(INNER), row(width), row(width),
            spec((8, INNER)), spec((INNER, width), **once), spec((8, 128)),
        ],
        out_specs=(
            row(width), spec((INNER, GROUP), lambda c: (0, c)), row(INNER), row(INNER), spec((STATE, INNER)),
            spec((8, INNER)),
        ),
        scratch_shapes=[pltpu.VMEM((STATE, INNER), F32)],
        compiler_params=params(),
        name="middle",
    )(y, reach, q, incoming, proj, hid, cot, gain, wout, flag)


def back_kernel(
    nz, x_ref, kq_ref, tailx_ref, tailkq_ref, tbx_ref, tbkq_ref, dcol_ref, ccol_ref, crow_ref, cm_ref, srow_ref,
    dy_ref, inc_ref, gcar_ref, one_ref, flag_ref, step_ref, it_ref, cot_ref,
    px_ref, pd_ref, head_ref, par_ref, gt_ref, last_ref, gout_ref,
    joined, joinedkq, kqc_s, kt_s, k_s, qt_s, q_s, s_s, bias_s, wb_s, wte_s, kg_s, qh_s, conv_s, hs_s, g_s, whole_s,
    ent_s, e_s, dcs, dst_s, dq_s, dk_s, r_s, rr_s, lt_s, ends_s,
    gcar_s, gsems, part_s, core_s, first_s, second_s, ring_s, send_sem, recv_sem,
):
    count = x_ref.shape[0]
    blocks = count // GROUP
    step = pl.program_id(0)
    lo = low_lanes(GROUP)
    eight = jnp.zeros((8, 128), F32)

    ticks = None
    if nz:
        p = Place(nz)
        steps = HEADS // HG
        w = part_s.shape[6]
        n_col = cot_ref.shape[1] // w
        jobs = it_ref.shape[1] * n_col
        deep = it_ref.shape[2]

        def gmoved(g):
            cols = pl.ds(pl.multiple_of(g * CG, CG), CG)
            return across(gcar_ref.at[:, cols], gcar_s.at[g], gsems, g)

        @pl.when(step == 0)
        def _():
            p.greet()
            gmoved(0).start()

        def job(j):
            col = pl.multiple_of(j % n_col * w, w)

            def out(total):
                gout_ref[pl.ds(pl.multiple_of(j // n_col * deep, deep), deep), pl.ds(col, w)] = total

            halves = [("x", 0, w // 2), ("y", w // 2, w)]
            got = [ref.at[j] for ref in (core_s, first_s, second_s, ring_s)]
            return Scatter(p, part_s.at[j], w, halves, got, (send_sem, recv_sem), (nz - 1 + 5) * j, out), col

        def ticks(t):
            for n, later in ((4, 6), (3, 5), (2, 3), (1, 1)):
                j = t - later

                @pl.when((j >= 0) & (j < jobs))
                def _(j=j, n=n):
                    job(j)[0].resume(n)

            @pl.when(t < jobs)
            def _():
                reduce, col = job(t)
                right = cot_ref[:, pl.ds(col, w)]
                for k in range(nz):
                    left = it_ref[k * 8 : k * 8 + 8, t // n_col].reshape(8 * deep, -1)
                    part_s[t, k] = dot(left, right).astype(BF).reshape(2, 2, 2, deep, w)
                reduce.resume(0)

        @pl.when(step < steps - 1)
        def _():
            gmoved(step + 1).start()

        ticks(2 * step)

    @pl.when(step == 0)
    def _():
        r_s[...] = jnp.zeros_like(r_s)
        rr_s[...] = jnp.zeros_like(rr_s)
        ends_s[...] = jnp.zeros_like(ends_s)
        lt_s[...] = jnp.zeros_like(lt_s)
        fill_joined(joinedkq, tailkq_ref, kq_ref)
        dst_s[...] = jnp.zeros_like(dst_s)
        dq_s[...] = jnp.zeros_like(dq_s)
        dk_s[...] = jnp.zeros_like(dk_s)

        @pl.loop(0, blocks)
        def _(c):
            base = pl.multiple_of(c * GROUP, GROUP)
            cm = cm_ref[pl.ds(base, GROUP), :]
            parts = []
            for half in range(2):
                conv = conv_block(joinedkq, base, slice(half * STATE, half * STATE + STATE), tbkq_ref, cm)
                kqc_s[pl.ds(base, GROUP), half * STATE : half * STATE + STATE] = conv
                parts.append(conv * jax.nn.sigmoid(conv))
            keys, queries = parts
            k_s[c] = keys.astype(BF)
            kt_s[c] = keys.T.astype(BF)
            q_s[c] = queries.astype(BF)
            qt_s[c] = queries.T.astype(BF)
            s_s[c] = dot(keys, queries, 1, 1, HIGHEST)
            bias_s[c] = bias_of(cm_ref, srow_ref, c, base, True)

    fill_joined(joined, tailx_ref, x_ref)
    par_col = pl.multiple_of(step * CG, CG)
    hs_s[0] = inc_ref[...].astype(F32) * flag_ref[0:1, 0:1]

    def expand(ccol, dcol, q):
        cum = [jnp.broadcast_to(ccol[:, h : h + 1], (GROUP, GROUP)) for h in (2 * q, 2 * q + 1)]
        dexp = jnp.where(lo, dcol[:, 2 * q : 2 * q + 1], dcol[:, 2 * q + 1 : 2 * q + 2])
        return cum, jnp.where(lo, cum[0], cum[1]), dexp

    @pl.loop(0, blocks)
    def _(c):
        base = pl.multiple_of(c * GROUP, GROUP)
        rows = pl.ds(base, GROUP)
        cm = cm_ref[rows, :]
        dcol, ccol = dcol_ref[0, rows, :], ccol_ref[0, rows, :]
        for q in range(HG // 2):
            lanes = slice(q * 128, q * 128 + 128)
            conv = conv_block(joined, base, lanes, tbx_ref, cm)
            conv_s[rows, lanes] = conv
            cum, cexp, dexp = expand(ccol, dcol, q)
            w = conv * jax.nn.sigmoid(conv) * dexp
            wb_s[rows, lanes] = w.astype(BF)
            end = cm[:, 5:6] * jnp.exp(cexp[GROUP - 1 :] - cexp)
            wte_s[rows, lanes] = (w * end).astype(BF)
            whole_s[c, 0:1, lanes] = cm[GROUP - 1 :, 4:5] * jnp.exp(cexp[GROUP - 1 :])
        hs_s[c + 1] = whole_s[c, 0:1, :] * hs_s[c] + dot(kt_s[c], wte_s[rows, :])

    if nz:
        gmoved(step).wait_recv()
        g_s[...] = gcar_s[step].astype(F32) * flag_ref[1:2, 0:1]
    else:
        g_s[...] = gcar_ref[...].astype(F32)
    dcs[0:8, :] = jnp.zeros((8, CG), F32)
    dcs[count + 8 :, :] = jnp.zeros((8, CG), F32)
    par_ref[:, pl.ds(par_col, CG)] = jnp.zeros((8, CG), F32)

    @pl.loop(0, blocks)
    def _(i):
        c = blocks - 1 - i
        if nz:

            @pl.when(i == blocks // 2)
            def _():
                ticks(2 * step + 1)

        base = pl.multiple_of(c * GROUP, GROUP)
        rows = pl.ds(base, GROUP)
        cm = cm_ref[rows, :]
        bias, scores = bias_s[c], s_s[c]
        dcol, ccol, crow = dcol_ref[0, rows, :], ccol_ref[0, rows, :], crow_ref[0, c]
        gb = g_s[...].astype(BF)
        kg_s[...] = dot(k_s[c], gb)
        hb = hs_s[c].astype(BF)
        qh_s[...] = dot(q_s[c], hb)
        gh = whole_s[c, 0:1, :] * jnp.sum(g_s[...] * hs_s[c], axis=0, keepdims=True)
        lane = lax.broadcasted_iota(jnp.int32, (GROUP, GROUP), 1)
        cols = jnp.zeros((GROUP, GROUP), F32)
        rows_of = [None] * HG
        for q in range(HG // 2):
            lanes = slice(q * 128, q * 128 + 128)
            conv = conv_s[rows, lanes]
            sg = jax.nn.sigmoid(conv)
            x = conv * sg
            cum, cexp, dexp = expand(ccol, dcol, q)
            dyb = dy_ref[rows, lanes]
            dy = dyb.astype(F32)
            wb = wb_s[rows, lanes]
            zero = jnp.zeros_like(dyb)
            spread = jnp.concatenate([jnp.where(lo, dyb, zero), jnp.where(lo, zero, dyb)], axis=0)
            dmat = dot(wb, spread, 1, 1)
            decay = [jnp.exp(crow[2 * q + i : 2 * q + i + 1] - cum[i] + bias) for i in range(2)]
            dst_s[c] += dmat[:, :GROUP] * decay[0] + dmat[:, GROUP:] * decay[1]
            mats = [d * scores for d in decay]
            for i in range(2):
                pairs = dmat[:, i * GROUP : (i + 1) * GROUP] * mats[i]
                cols = jnp.where(lane == step * HG + 2 * q + i, jnp.sum(pairs, axis=1, keepdims=True), cols)
                rows_of[2 * q + i] = jnp.sum(pairs, axis=0, keepdims=True)
            mats = jnp.concatenate([m.astype(BF) for m in mats], axis=1)
            end = cm[:, 5:6] * jnp.exp(cexp[GROUP - 1 :] - cexp)
            enter = cm[:, 4:5] * jnp.exp(cexp)
            kge = end * kg_s[:, lanes]
            dw = dot(mats, spread) + kge
            edy = enter * dy
            ent_s[:, lanes] = edy.astype(BF)
            kge = wb.astype(F32) * kge
            lt_s[pl.ds(c * 8, 1), lanes] = gh[:, lanes] + jnp.sum(kge, axis=0, keepdims=True)
            skip = tbx_ref[5:6, lanes]
            skx = dy * x
            for n, e in enumerate((edy * qh_s[:, lanes] - kge, x * dw)):
                high = e.astype(BF)
                e_s[0, :, n * CG + q * 128 : n * CG + q * 128 + 128] = high
                e_s[1, :, n * CG + q * 128 : n * CG + q * 128 + 128] = (e - high.astype(F32)).astype(BF)
            dconv = (dexp * dw + skip * dy) * (sg * (1.0 + conv * (1.0 - sg)))
            dcs[pl.ds(base + 8, GROUP), lanes] = dconv
            block = joined[pl.ds(base, GROUP + 8), lanes]
            sums = [
                jnp.sum(dconv * (shifted(block, 5 + k, GROUP) * cm[:, k : k + 1]), axis=0, keepdims=True)
                for k in range(CONV)
            ]
            sums += [jnp.sum(dconv, axis=0, keepdims=True), jnp.sum(skx, axis=0, keepdims=True)]
            par_ref[:, pl.ds(par_col + q * 128, 128)] += jnp.concatenate(sums + [eight[:2]], axis=0)
        entb = ent_s[...]
        dq_s[c] += dot(entb, hb, 1, 1)
        dk_s[c] += dot(wte_s[rows, :], gb, 1, 1)
        g_s[...] = whole_s[c, 0:1, :] * g_s[...] + dot(qt_s[c], entb)
        r_s[rows, :] += dot(e_s[0], one_ref[0]) + dot(e_s[1], one_ref[0]) - cols
        rr_s[c, pl.ds(pl.multiple_of(step * HG, HG), HG), :] = jnp.concatenate(rows_of, axis=0)

    def unconv(dcs_ref, tb_ref, width, col):
        for q in range(width // 128):
            lanes = slice(q * 128, q * 128 + 128)
            cols = pl.ds(col + q * 128, 128)

            def pull(start, rows, cm_start):
                block = dcs_ref[pl.ds(start, rows + 8), lanes]
                cm = cm_ref[pl.ds(cm_start, rows + 8), :]
                total = jnp.zeros((rows, 128), F32)
                for k in range(CONV):
                    total = total + tb_ref[k : k + 1, lanes] * shifted(block * cm[:, k : k + 1], 3 - k, rows)
                return total

            @pl.loop(0, blocks)
            def _(c):
                base = pl.multiple_of(c * GROUP, GROUP)
                got = pull(base + 8, GROUP, base)
                px_ref[pl.ds(base, GROUP), cols] = got.astype(BF)
                last_ref[:, cols] = got[GROUP - 8 :]

            block = jnp.concatenate([jnp.zeros((8, 128), F32), dcs_ref[8:16, lanes]], axis=0)
            cm = jnp.concatenate([jnp.zeros((8, 8), F32), cm_ref[0:8, :]], axis=0)
            total = jnp.zeros((8, 128), F32)
            for k in range(CONV):
                total = total + tb_ref[k : k + 1, lanes] * shifted(block * cm[:, k : k + 1], 3 - k, 8)
            gt_ref[:, cols] = total

    unconv(dcs, tbx_ref, CG, par_col)
    low = lt_s[...]
    high = low.astype(BF)
    ends_s[...] += dot(high, one_ref[0, :CG]) + dot((low - high.astype(F32)).astype(BF), one_ref[0, :CG])

    @pl.when(step == pl.num_programs(0) - 1)
    def _():
        par_ref[:, INNER:] = jnp.zeros((8, 2 * STATE), F32)

        @pl.loop(0, blocks)
        def _(c):
            base = pl.multiple_of(c * GROUP, GROUP)
            rows = pl.ds(base, GROUP)
            cm = cm_ref[rows, :]
            dst = dst_s[c]
            dk = dk_s[c] + dot(dst.astype(BF), q_s[c])
            dq = dq_s[c] + dot(dst.T.astype(BF), k_s[c])
            for half, grad in enumerate((dk, dq)):
                lanes = slice(half * STATE, half * STATE + STATE)
                conv = kqc_s[rows, lanes]
                sg = jax.nn.sigmoid(conv)
                dconv = grad * (sg * (1.0 + conv * (1.0 - sg)))
                dcs[pl.ds(base + 8, GROUP), lanes] = dconv
                block = joinedkq[pl.ds(base, GROUP + 8), lanes]
                sums = [
                    jnp.sum(dconv * (shifted(block, 5 + k, GROUP) * cm[:, k : k + 1]), axis=0, keepdims=True)
                    for k in range(CONV)
                ]
                sums += [jnp.sum(dconv, axis=0, keepdims=True)]
                par_ref[:, INNER + half * STATE : INNER + half * STATE + STATE] += jnp.concatenate(
                    sums + [eight[:3]], axis=0
                )

        unconv(dcs, tbkq_ref, 2 * STATE, INNER)
        down = lax.broadcasted_iota(jnp.int32, (GROUP, GROUP), 0)
        over = lax.broadcasted_iota(jnp.int32, (GROUP, GROUP), 1)
        later = jnp.where(over >= down, 1.0, 0.0)
        head_ref[...] = jnp.zeros_like(head_ref)

        @pl.loop(0, blocks)
        def _(c):
            rows = pl.ds(pl.multiple_of(c * GROUP, GROUP), GROUP)
            both = r_s[rows, :]
            grown = dot(later, both + rr_s[c].T, precision=HIGHEST) + ends_s[pl.ds(c * 8, 1), :]
            grown = jnp.where(over < HEADS, grown, 0.0)
            direct = pltpu.roll(both, 64, 1)
            dstep = (direct - flag_ref[2:3, :] * grown) * step_ref[1, rows, :]
            pd_ref[rows, :] = dstep.astype(BF)
            head_ref[0:1, :] += jnp.sum(grown * step_ref[0, rows, :], axis=0, keepdims=True)
            head_ref[1:2, :] += jnp.sum(dstep, axis=0, keepdims=True)

        if nz:
            for g in range(HEADS // HG):
                gmoved(g).wait_send()


def back(xz, xoff, tail, tb, dcol, ccol, crow, cm, srow, dy, incoming, gcar, one, flag, step, inner_t, cot, nz):
    count = xz.shape[0]
    blocks = count // GROUP
    steps = HEADS // HG
    vm = pltpu.VMEM
    dma = pltpu.SemaphoreType.DMA
    hbm = pl.BlockSpec(memory_space=pl.ANY)
    if nz:
        parts = inner_t.shape[0] // cot.shape[1]
        deep = inner_t.shape[0] // (8 * nz * parts)
        jobs = parts * (cot.shape[1] // CG)
        shape = (parts * deep, cot.shape[1])
    else:
        parts, deep, jobs, shape = 1, 8, 1, (8, 128)
        inner_t, cot = jnp.zeros((8, 128), BF), jnp.zeros((8, 128), BF)
    mid = max(nz, 1)
    inner_t = inner_t.reshape((8 * nz, parts, deep, -1) if nz else (1, 1, 8, 128))
    return pl.pallas_call(
        functools.partial(back_kernel, nz),
        grid=(steps,),
        out_shape=(
            jax.ShapeDtypeStruct((count, XBC), BF),
            jax.ShapeDtypeStruct((count, 128), BF),
            jax.ShapeDtypeStruct((8, 128), F32),
            jax.ShapeDtypeStruct((8, XBC), F32),
            jax.ShapeDtypeStruct((8, XBC), F32),
            jax.ShapeDtypeStruct((8, XBC), F32),
            jax.ShapeDtypeStruct(shape, F32),
        ),
        in_specs=[
            spec((count, CG), lambda g: (0, xoff // CG + g)),
            spec((count, 2 * STATE), lambda g: (0, (xoff + INNER) // (2 * STATE))),
            spec((8, CG), lambda g: (0, g)),
            spec((8, 2 * STATE), lambda g: (0, INNER // (2 * STATE))),
            spec((8, CG), lambda g: (0, g)),
            spec((8, 2 * STATE), lambda g: (0, INNER // (2 * STATE))),
            spec((1, count, HG), lambda g: (g, 0, 0)),
            spec((1, count, HG), lambda g: (g, 0, 0)),
            spec((1, blocks, HG, GROUP), lambda g: (g, 0, 0, 0)),
            spec((count + 8, 8)),
            spec((blocks, 8, GROUP)),
            spec((count, CG), lambda g: (0, g)),
            spec((STATE, CG), lambda g: (0, g)),
            hbm if nz else spec((STATE, CG), lambda g: (0, g)),
            spec((1, 2 * CG, 128), lambda g: (g, 0, 0)),
            spec((8, 128)),
            spec((2, count, 128)),
            spec(inner_t.shape, pipeline_mode=pl.Buffered(1)),
            spec(cot.shape, pipeline_mode=pl.Buffered(1)),
        ],
        out_specs=(
            spec((count, XBC)),
            spec((count, 128)),
            spec((8, 128)),
            spec((8, XBC)),
            spec((8, XBC)),
            spec((8, XBC)),
            spec(shape),
        ),
        scratch_shapes=[
            vm((count + 8, CG), F32),
            vm((count + 8, 2 * STATE), F32),
            vm((count, 2 * STATE), F32),
            vm((blocks, STATE, GROUP), BF),
            vm((blocks, GROUP, STATE), BF),
            vm((blocks, STATE, GROUP), BF),
            vm((blocks, GROUP, STATE), BF),
            vm((blocks, GROUP, GROUP), F32),
            vm((blocks, GROUP, GROUP), F32),
            vm((count, CG), BF),
            vm((count, CG), BF),
            vm((GROUP, CG), F32),
            vm((GROUP, CG), F32),
            vm((count, CG), F32),
            vm((blocks + 1, STATE, CG), F32),
            vm((STATE, CG), F32),
            vm((blocks, 8, CG), F32),
            vm((GROUP, CG), BF),
            vm((2, GROUP, 2 * CG), BF),
            vm((count + 16, CG), F32),
            vm((blocks, GROUP, GROUP), F32),
            vm((blocks, GROUP, STATE), F32),
            vm((blocks, GROUP, STATE), F32),
            vm((count, 128), F32),
            vm((blocks, 128, GROUP), F32),
            vm((8 * blocks, CG), F32),
            vm((8 * blocks, 128), F32),
            vm((steps, STATE, CG), BF),
            dma((2, steps)),
            vm((jobs, mid, 2, 2, 2, deep, CG), BF),
            vm((jobs, mid, 2, 2, deep, CG), BF),
            vm((jobs, 2, mid, 2, deep, CG // 2), BF),
            vm((jobs, 2, mid, deep, CG // 2), BF),
            vm((jobs, max(mid - 1, 1), deep, CG), BF),
            dma((jobs * (mid + 4),)),
            dma((jobs * (mid + 4),)),
        ],
        compiler_params=params(**(dict(collective_id=4, has_side_effects=True) if nz else {})),
        name="mixer_back",
    )(
        xz, xz, tail, tail, tb, tb, dcol, ccol, crow, cm, srow, dy, incoming, gcar, one, flag, step, inner_t, cot
    )


MESH = pl.DeviceIdType.MESH


class Place:
    def __init__(self, nz):
        dp, self.x = lax.axis_index("dp"), lax.axis_index("seq")
        self.c, self.y, self.z, self.nz = dp % 2, (dp // 2) % 2, dp // 4, nz

    def at(self, z, y, c, x):
        return {"dp": (z * 2 + y) * 2 + c, "seq": x}

    def up(self, r):
        return self.at((self.z + r) % self.nz, self.y, self.c, self.x)

    def flip(self, axis):
        return self.at(
            self.z,
            1 - self.y if axis == "y" else self.y,
            1 - self.c if axis == "c" else self.c,
            1 - self.x if axis == "x" else self.x,
        )

    def greet(self):
        barrier = pltpu.get_barrier_semaphore()
        others = [self.up(r) for r in range(1, self.nz)] + [self.flip(a) for a in "yxc"]
        for other in others:
            pl.semaphore_signal(barrier, inc=1, device_id=other, device_id_type=MESH)
        pl.semaphore_wait(barrier, len(others))


def columns_of(width, tiles):
    total, groups, start = width // 128, [], 0
    while start < total:
        size = min(tiles, total - start)
        if total - start - size == 1:
            size += 1
        groups.append((start * 128, (start + size // 2) * 128, (start + size) * 128))
        start += size
    return groups


def send(src, dst, sems, slot, device):
    copy = pltpu.make_async_remote_copy(
        src_ref=src, dst_ref=dst, send_sem=sems[0].at[slot], recv_sem=sems[1].at[slot],
        device_id=device, device_id_type=MESH,
    )
    copy.start()
    return copy


class Gather:
    def __init__(self, place, ref, cut, sems, first):
        self.p, self.ref, self.cut, self.sems, self.first = place, ref, cut, sems, first
        self.copies = []

    @property
    def slots(self):
        return self.p.nz - 1 + 5

    def push(self, index, slot, device):
        ref = self.ref.at[index]
        copy = send(ref, ref, self.sems, self.first + slot, device)
        self.copies.append(copy)
        return copy

    def phase(self, n):
        p, (a, m, b) = self.p, self.cut
        every, k = slice(None), self.p.nz - 1
        if n == 0:
            self.last = [self.push((p.z, p.y, p.c, p.x, every, slice(a, b)), r - 1, p.up(r)) for r in range(1, p.nz)]
            return
        for copy in self.last:
            copy.wait_recv()
        if n == 1:
            self.last = [
                self.push((every, p.y, p.c, p.x, every, slice(a, m)), k, p.flip("y")),
                self.push((every, p.y, p.c, p.x, every, slice(m, b)), k + 1, p.flip("x")),
            ]
        elif n == 2:
            self.last = [
                self.push((every, every, p.c, p.x, every, slice(a, m)), k + 2, p.flip("x")),
                self.push((every, p.y, p.c, every, every, slice(m, b)), k + 3, p.flip("y")),
            ]
        elif n == 3:
            self.last = [self.push((every, every, p.c, every, every, slice(a, b)), k + 4, p.flip("c"))]

    def drain(self):
        for copy in self.copies:
            copy.wait_send()


def gather_kernel(
    nz, tiles, win_ref, wout_ref, small_ref, hid_ref,
    full_ref, wfull_ref, sfull_ref, normed_ref, normed_t_ref, proj_ref,
    wbuf, obuf, sbuf, send_sem, recv_sem, own_sem, out_sem,
):
    p = Place(nz)
    own = []
    for i, (src, buf) in enumerate(((small_ref, sbuf), (win_ref, wbuf), (wout_ref, obuf))):
        own.append(pltpu.make_async_copy(src, buf.at[p.z, p.y, p.c, p.x], own_sem.at[i]))
        own[-1].start()
    p.greet()
    jobs = [(sbuf, cut, "small") for cut in columns_of(small_ref.shape[1], small_ref.shape[1] // 128)]
    jobs += [(wbuf, cut, "in") for cut in columns_of(win_ref.shape[1], tiles)]
    jobs += [(obuf, cut, "out") for cut in columns_of(wout_ref.shape[1], tiles // 2 + tiles % 2)]
    per = nz - 1 + 5
    gathers = [Gather(p, buf, cut, (send_sem, recv_sem), per * i) for i, (buf, cut, _) in enumerate(jobs)]
    for copy in own:
        copy.wait()
    outs = []

    def finish(i):
        buf, (a, _, b), kind = jobs[i]
        gathers[i].phase(4)
        if kind == "small":
            gain = jnp.sum(sbuf[...].astype(F32), axis=(0, 1, 2, 3))[0:1]
            rows = hid_ref[...].astype(F32)
            scale = lax.rsqrt(jnp.mean(rows * rows, axis=1, keepdims=True) + norm_eps)
            normed = (rows * scale * gain).astype(BF)
            normed_ref[...] = normed
            normed_t_ref[...] = normed.T
        target = {"small": sfull_ref, "in": full_ref, "out": wfull_ref}[kind]
        every = (slice(None),) * 5
        copy = pltpu.make_async_copy(buf.at[every + (slice(a, b),)], target.at[every + (slice(a, b),)], out_sem.at[i])
        copy.start()
        outs.append(copy)
        if kind == "in":
            weights = buf[:, :, :, :, :, a:b].reshape(-1, b - a)
            proj_ref[:, a:b] = dot(normed_ref[...], weights).astype(BF)

    gathers[0].phase(0)
    for tick in range(len(jobs) + 3):
        if tick + 1 < len(jobs):
            gathers[tick + 1].phase(0)
        for back, n in ((0, 1), (1, 2), (2, 3)):
            if 0 <= tick - back < len(jobs):
                gathers[tick - back].phase(n)
        if tick >= 3:
            finish(tick - 3)
    for g in gathers:
        g.drain()
    for copy in outs:
        copy.wait()


def gather(win, wout, small, hid, nz, tiles=4):
    count, width = hid.shape
    whole = lambda a: jax.ShapeDtypeStruct((nz, 2, 2, 2) + a.shape, BF)
    jobs = 1 + len(columns_of(win.shape[1], tiles)) + len(columns_of(wout.shape[1], tiles // 2 + tiles % 2))
    slots = jobs * (nz - 1 + 5)
    hbm = pl.BlockSpec(memory_space=pl.ANY)
    vmem = pl.BlockSpec(memory_space=pltpu.VMEM)
    dma = pltpu.SemaphoreType.DMA
    full, wfull, sfull, _, normed_t, proj = pl.pallas_call(
        functools.partial(gather_kernel, nz, tiles),
        out_shape=(
            whole(win), whole(wout), whole(small),
            jax.ShapeDtypeStruct((count, width), BF),
            jax.ShapeDtypeStruct((width, count), BF),
            jax.ShapeDtypeStruct((count, win.shape[1]), BF),
        ),
        in_specs=[hbm, hbm, hbm, vmem],
        out_specs=(hbm, hbm, hbm, vmem, vmem, vmem),
        scratch_shapes=[
            pltpu.VMEM(whole(win).shape, BF), pltpu.VMEM(whole(wout).shape, BF), pltpu.VMEM(whole(small).shape, BF),
            dma((slots,)), dma((slots,)), dma((3,)), dma((jobs,)),
        ],
        compiler_params=params(collective_id=1, has_side_effects=True),
        name="gather_project",
    )(win, wout, small, hid)
    return full, wfull.reshape(-1, wout.shape[1]), sfull, normed_t, proj


class Scatter:
    def __init__(self, place, part, width, halves, got, sems, first, out):
        self.p, self.part, self.width, self.halves = place, part, width, halves
        self.got, self.sems, self.first, self.out = got, sems, first, out

    def add(self, index, got):
        self.part[index] = (self.part[index].astype(F32) + got.astype(F32)).astype(self.part.dtype)

    def copies(self, n):
        p, every, k = self.p, slice(None), self.p.nz - 1
        z, y, c, x = p.z, p.y, p.c, p.x
        cols = slice(0, self.width)
        core, first, second, ring = self.got
        found = []

        def push(index, dst, slot, device):
            found.append(
                pltpu.make_async_remote_copy(
                    src_ref=self.part.at[index], dst_ref=dst, send_sem=self.sems[0].at[self.first + slot],
                    recv_sem=self.sems[1].at[self.first + slot], device_id=device, device_id_type=MESH,
                )
            )

        if n == 0:
            push((every, every, 1 - c, every, every, cols), core.at[..., cols], k + 4, p.flip("c"))
        elif n == 1:
            for i, (axis, lo, hi) in enumerate(self.halves):
                index = (every, every, c, 1 - x) if axis == "x" else (every, 1 - y, c, every)
                push(index + (every, slice(lo, hi)), first.at[i, :, :, :, 0 : hi - lo], k + i, p.flip(axis))
        elif n == 2:
            for i, (axis, lo, hi) in enumerate(self.halves):
                index = (every, 1 - y, c, x) if axis == "x" else (every, y, c, 1 - x)
                other = p.flip("y" if axis == "x" else "x")
                push(index + (every, slice(lo, hi)), second.at[i, :, :, 0 : hi - lo], k + 2 + i, other)
        elif n == 3:
            for r in range(1, p.nz):
                push((lax.rem(z + r, p.nz), y, c, x, every, cols), ring.at[r - 1, :, cols], r - 1, p.up(r))
        return found

    def resume(self, n):
        p, every = self.p, slice(None)
        z, y, c, x = p.z, p.y, p.c, p.x
        cols = slice(0, self.width)
        core, first, second, ring = self.got
        if n > 0:
            for copy in self.copies(n - 1):
                copy.wait_recv()
        if n == 1:
            for i in range(p.nz):
                self.add((i, every, c, every, every, cols), core[i, :, :, :, cols])
        elif n == 2:
            for i, (axis, lo, hi) in enumerate(self.halves):
                index = (every, every, c, x) if axis == "x" else (every, y, c, every)
                self.add(index + (every, slice(lo, hi)), first[i, :, :, :, 0 : hi - lo])
        elif n == 3:
            for i, (axis, lo, hi) in enumerate(self.halves):
                self.add((every, y, c, x, every, slice(lo, hi)), second[i, :, :, 0 : hi - lo])
        elif n == 4:
            total = self.part[z, y, c, x, :, cols].astype(F32)
            for r in range(p.nz - 1):
                total = total + ring[r, :, cols].astype(F32)
            self.out(total)
            for m in range(4):
                for copy in self.copies(m):
                    copy.wait_send()
            return
        for copy in self.copies(n):
            copy.start()


RING = 5


def scatter_kernel(
    nz, tiles,
    nt_ref, cot_ref, pz_ref, px_ref, pd_ref, full_ref, hid_ref, gain_ref, small_ref, gt_ref, last_ref,
    gin_ref, gsmall_ref, ng_ref,
    part_big, part_small, core_big, core_small, first_big, first_small, second_big, second_small,
    ring_big, ring_small, wbuf, gbuf, tails, patch, send_sem, recv_sem, w_sem, g_sem, t_sems,
):
    p = Place(nz)
    per = nz - 1 + 5
    cuts = columns_of(full_ref.shape[5], tiles)
    jobs = [("in", cut) for cut in cuts] + [("small", (0, 128, 128))]
    n_in = len(cuts)
    deep = nt_ref.shape[0] // (8 * nz)
    every = (slice(None),) * 5

    class Fetch:
        def __init__(self, i):
            a, _, b = cuts[i]
            self.copies = [
                pltpu.make_async_copy(
                    full_ref.at[every + (slice(a, b),)], wbuf.at[i % 2, :, :, :, :, :, 0 : b - a], w_sem.at[i % 2]
                )
            ]
            start = 0
            for n, ref in enumerate((pz_ref, px_ref, pd_ref)):
                lo, hi = max(a, start), min(b, start + ref.shape[1])
                if lo < hi:
                    self.copies.append(
                        pltpu.make_async_copy(
                            ref.at[:, lo - start : hi - start], gbuf.at[i % 2, :, lo - a : hi - a], g_sem.at[i % 2, n]
                        )
                    )
                start += ref.shape[1]

        def start(self):
            for copy in self.copies:
                copy.start()

        def wait(self):
            for copy in self.copies:
                copy.wait()

    fetches = [Fetch(i) for i in range(n_in)]
    fetches[0].start()
    tails[0] = gt_ref[...].astype(BF)
    p.greet()
    tail_copy = across(tails.at[0], tails.at[1], t_sems, 0)
    tail_copy.start()
    scatters = []
    for i, (kind, (a, m, b)) in enumerate(jobs):
        if kind == "small":
            part, got, n = part_small, (core_small, first_small, second_small, ring_small), 0
        else:
            part, got, n = part_big.at[i % RING], (core_big, first_big, second_big, ring_big), i
        halves = [("x", 0, m - a)] + ([("y", m - a, b - a)] if b > m else [])

        def out(total, kind=kind, a=a, b=b):
            {"in": gin_ref, "small": gsmall_ref}[kind][:, a:b] = total

        scatters.append(
            Scatter(
                p, part, b - a, halves, [g.at[n] for g in got], (send_sem, recv_sem), per * i, out
            )
        )

    done = {"in": 0}

    def fill(i):
        kind, (a, _, b) = jobs[i]
        if kind == "small":
            rows = hid_ref[...].astype(F32)
            scale = lax.rsqrt(jnp.mean(rows * rows, axis=1, keepdims=True) + norm_eps)
            unit = rows * scale
            grad = ng_ref[...]
            gpre = jnp.sum(grad * unit, axis=0, keepdims=True)
            grad = grad * gain_ref[0:1, :]
            grad = scale * (grad - unit * jnp.mean(grad * unit, axis=1, keepdims=True))
            ng_ref[...] = cot_ref[...].astype(F32) + grad
            gpre = jnp.broadcast_to(gpre, (8, gpre.shape[1]))
            share = gpre.shape[1] // (8 * nz)
            part_small[...] = small_ref[...]
            for j in range(8 * nz):
                moved = gpre if j == 0 else pltpu.roll(gpre, gpre.shape[1] - share * j, 1)
                part_small[j // 8, j // 4 % 2, j // 2 % 2, j % 2, 7:8, :] = moved[0:1, :128]
            return
        part = scatters[i].part
        high = deep * 8
        n = done["in"]
        done["in"] += 1
        fetches[n].wait()
        if n + 1 < n_in:
            fetches[n + 1].start()
        lo, hi = max(a, pz_ref.shape[1]), min(b, pz_ref.shape[1] + px_ref.shape[1])
        if lo < hi:
            if not done.get("tail"):
                done["tail"] = True
                tail_copy.wait()
                keep = jnp.where(p.x == 0, 1.0, 0.0)
                patch[...] = (last_ref[...] + keep * tails[1].astype(F32)).astype(BF)
            start = pz_ref.shape[1]
            gbuf[n % 2, -8:, lo - a : hi - a] = patch[:, lo - start : hi - start]
        right = gbuf[n % 2, :, 0 : b - a]
        for k in range(nz):
            left = nt_ref[k * high : (k + 1) * high, :]
            block = dot(left, right).astype(BF)
            part[k, :, :, :, :, 0 : b - a] = block.reshape(2, 2, 2, deep, b - a)

    def pull(i):
        kind, (a, _, b) = jobs[i]
        if kind == "in":
            n = done["in"] - 1
            weights = wbuf[n % 2, :, :, :, :, :, 0 : b - a].reshape(-1, b - a)
            grown = dot(gbuf[n % 2, :, 0 : b - a], weights, 1, 1)
            if n == 0:
                ng_ref[...] = grown
            else:
                ng_ref[...] += grown

    for tick in range(len(jobs) + 4):
        for back in (4, 3, 2, 1):
            if 0 <= tick - back < len(jobs):
                scatters[tick - back].resume(back)
        if tick < len(jobs):
            fill(tick)
            scatters[tick].resume(0)
            pull(tick)


def scatter(normed_t, cot, pz, px, pd, full, hid, gain, small, gt, last, nz, tiles=4):
    rows_in = normed_t.shape[0] // (8 * nz)
    width_in = pz.shape[1] + px.shape[1] + pd.shape[1]
    n_in = len(columns_of(width_in, tiles))
    hbm = pl.BlockSpec(memory_space=pl.ANY)
    vmem = pl.BlockSpec(memory_space=pltpu.VMEM)
    dma = pltpu.SemaphoreType.DMA
    vm = pltpu.VMEM
    w = tiles * 128
    shapes = [(n_in, rows_in, w, BF), (1, 8, 128, F32)]
    parts = [vm((RING, nz, 2, 2, 2, rows_in, w), BF), vm((nz, 2, 2, 2, 8, 128), F32)]
    core = [vm((n, nz, 2, 2, r, w), t) for n, r, w, t in shapes]
    first = [vm((n, 2, nz, 2, r, max(w // 2, 128)), t) for n, r, w, t in shapes]
    second = [vm((n, 2, nz, r, max(w // 2, 128)), t) for n, r, w, t in shapes]
    ring = [vm((n, nz - 1, r, w), t) for n, r, w, t in shapes]
    slots = (n_in + 1) * (nz - 1 + 5)
    return pl.pallas_call(
        functools.partial(scatter_kernel, nz, tiles),
        out_shape=(
            jax.ShapeDtypeStruct((rows_in, width_in), F32),
            jax.ShapeDtypeStruct((8, 128), F32),
            jax.ShapeDtypeStruct(hid.shape, F32),
        ),
        in_specs=[vmem] * 2 + [hbm] * 4 + [vmem] * 5,
        out_specs=(vmem,) * 3,
        scratch_shapes=parts + core + first + second + ring + [
            vm((2, nz, 2, 2, 2, rows_in, w), BF), vm((2, cot.shape[0], w), BF), vm((2,) + gt.shape, BF), vm(gt.shape, BF),
            dma((slots,)), dma((slots,)), dma((2,)), dma((2, 3)), dma((2, 1)),
        ],
        compiler_params=pltpu.CompilerParams(
            vmem_limit_bytes=67043328, collective_id=2, has_side_effects=True
        ),
        name="grads_scatter",
    )(normed_t, cot, pz, px, pd, full, hid, gain, small, gt, last)


def passed_along(shard, axis, by):
    count = lax.axis_size(axis)
    pairs = [(i, i + by) for i in range(count) if 0 <= i + by < count]
    return lax.ppermute(shard, axis, pairs)


def chained(own, factor, axis, by):
    got = jnp.zeros(own.shape, BF)
    for i in range(lax.axis_size(axis) - 1):
        sent = own if i == 0 else own.astype(F32) + factor * got.astype(F32)
        got = passed_along(sent.astype(BF), axis, by)
    return got


def adamw(weight, grad, mean, square, rate, decay):
    new_mean = first_beta * mean + (1.0 - first_beta) * grad
    new_square = second_beta * square + (1.0 - second_beta) * grad * grad
    corrected = new_mean / (1.0 - first_beta**STEP)
    spread = jnp.sqrt(new_square / (1.0 - second_beta**STEP))
    new_weight = weight * (1.0 - rate * decay) - rate * corrected / (spread + adam_eps)
    return (new_weight, new_mean, new_square)


def prepare(step_raw, seg_ext, step_bias, decay_log):
    count = step_raw.shape[0]
    blocks, steps = count // GROUP, HEADS // HG
    delta = jax.nn.softplus(step_raw + step_bias[None, :])
    logdec = -delta * jnp.exp(decay_log)[None, :]
    lower = jnp.tril(jnp.ones((GROUP, GROUP), F32))
    cum = jnp.einsum("ij,cjh->cih", lower, logdec.reshape(blocks, GROUP, HEADS), precision=HIGHEST)
    own = seg_ext[CONV - 1 :]
    seg_blocks = own.reshape(blocks, GROUP)
    before = jnp.concatenate([seg_ext[CONV - 2 : CONV - 1], seg_blocks[:-1, -1]])
    columns = [seg_ext[k : k + count] == own for k in range(CONV)]
    columns += [(seg_blocks == before[:, None]).reshape(count), (seg_blocks == seg_blocks[:, -1:]).reshape(count)]
    columns = [c.astype(F32) for c in columns] + [own.astype(F32), jnp.zeros((count,), F32)]
    cm = jnp.pad(jnp.stack(columns, axis=1), ((0, 8), (0, 0)))
    srow = jnp.broadcast_to(seg_blocks.astype(F32)[:, None, :], (blocks, 8, GROUP))
    dcol = delta.reshape(count, steps, HG).transpose(1, 0, 2)
    ccol = cum.reshape(count, steps, HG).transpose(1, 0, 2)
    crow = cum.reshape(blocks, GROUP, steps, HG).transpose(2, 0, 3, 1)
    return delta, logdec, (dcol, ccol, crow, cm, srow)


def shards(
    hidden,
    cotangent,
    segments,
    weight_in,
    weight_out,
    gain_pre,
    gain_gated,
    conv_taps,
    conv_bias,
    decay_log,
    skip_gain,
    step_bias,
    mean_weight_in,
    square_weight_in,
    mean_weight_out,
    square_weight_out,
    mean_gain_pre,
    square_gain_pre,
    mean_gain_gated,
    square_gain_gated,
    mean_conv_taps,
    square_conv_taps,
    mean_conv_bias,
    square_conv_bias,
    mean_decay_log,
    square_decay_log,
    mean_skip_gain,
    square_skip_gain,
    mean_step_bias,
    square_step_bias,
):
    piece = hidden.shape[1]
    blocks, steps = piece // GROUP, HEADS // HG
    devices = lax.axis_size("dp") * lax.axis_size("seq")
    offset = lax.axis_index("seq") * piece
    lead = jnp.full((CONV - 1,), -1, jnp.int32)
    seg_ext = lax.dynamic_slice_in_dim(jnp.concatenate([lead, segments[0]]), offset, piece + CONV - 1)

    sizes = (gain_pre.shape[0], gain_gated.shape[0], conv_taps.size, conv_bias.shape[0])
    small = jnp.concatenate([gain_pre, gain_gated, conv_taps.reshape(-1), conv_bias]).astype(BF)
    me = lax.axis_index("dp") * lax.axis_size("seq") + lax.axis_index("seq")
    width = hidden.shape[2]
    padded = -(-weight_in.shape[1] // 128) * 128
    win_low = jnp.pad(weight_in.astype(BF), ((0, 0), (0, padded - weight_in.shape[1])))
    rows = hidden[0].astype(F32)
    scale = lax.rsqrt(jnp.mean(rows * rows, axis=-1, keepdims=True) + norm_eps)
    nz = lax.axis_size("dp") // 4
    own = weight_in.shape[0] % 16 == 0 and lax.axis_size("seq") == 2 and lax.axis_size("dp") == 4 * nz
    if own:
        placed = lax.dynamic_update_slice_in_dim(jnp.zeros((width,), BF), gain_pre.astype(BF), me * sizes[0], 0)
        block = jnp.stack([placed, jnp.pad(small, (0, width - small.shape[0]))])
        block = jnp.pad(block, ((0, 6), (0, 0)))
        full, w_out, small, normed_t, proj = gather(win_low, weight_out.astype(BF), block, hidden[0], nz)
        small = small.reshape(devices, 8, width)[:, 1, : sum(sizes)].astype(F32)
    else:
        small = lax.all_gather(small, BOTH, axis=0).astype(F32)
        w_in = lax.all_gather(win_low, BOTH, axis=0, tiled=True)
        w_out = lax.all_gather(weight_out.astype(BF), BOTH, axis=0, tiled=True)
    cuts = [0]
    for s in sizes:
        cuts.append(cuts[-1] + s)
    pre_gain, gated_gain, taps, cbias = [small[:, a:b] for a, b in zip(cuts, cuts[1:])]
    pre_gain, gated_gain, cbias = pre_gain.reshape(-1), gated_gain.reshape(-1), cbias.reshape(-1)
    taps = taps.reshape(devices, CONV, -1).transpose(1, 0, 2).reshape(CONV, XBC)

    if not own:
        normed = (rows * scale * pre_gain).astype(BF)
        proj = jnp.dot(normed, w_in, preferred_element_type=F32).astype(BF)
    tail = passed_along(proj[piece - CONV + 1 :, INNER : INNER + XBC], "seq", 1)
    tail = jnp.pad(tail, ((8 - CONV + 1, 0), (0, 0)))
    skip_lanes = jnp.pad(jnp.repeat(skip_gain, HEAD_DIM), (0, XBC - INNER))
    tb = jnp.concatenate([taps, cbias[None], skip_lanes[None], jnp.zeros((2, XBC), F32)])
    step_raw = proj[:, INNER + XBC : INNER + XBC + HEADS].astype(F32)
    delta, logdec, prepared = prepare(step_raw, seg_ext, step_bias, decay_log)

    remote = nz if own else 0
    mixed, reach, queries, carried, passed = front(proj, INNER, tail, tb, *prepared, own)
    incoming = carried if own else chained(carried, passed[:1], "seq", 1)
    gain8 = jnp.broadcast_to(gated_gain[None], (8, INNER))
    place, count_seq = lax.axis_index("seq"), lax.axis_size("seq")
    lane = lambda v: jnp.pad(v, [(0, 0)] * (v.ndim - 1) + [(0, 128 - HEADS)])
    before, after = jnp.where(place > 0, 1.0, 0.0), jnp.where(place < count_seq - 1, 1.0, 0.0)
    flag = jnp.stack([jnp.full((128,), before), jnp.full((128,), after), lane(jnp.exp(decay_log))])
    flag = jnp.pad(flag.astype(F32), ((0, 5), (0, 0)))
    output, inner_t, dy, dz, ginc, ggain = middle(
        mixed, reach, queries, incoming, proj, hidden[0], cotangent[0], gain8, w_out, flag
    )
    grad_gated = ggain[0]
    gcar = ginc if own else chained(ginc, passed[:1], "seq", -1)
    channel = jnp.arange(2 * CG)[None, :, None]
    goal = jnp.arange(steps)[:, None, None] * HG + channel % CG // HEAD_DIM + channel // CG * 64
    one = (goal == jnp.arange(128)[None, None, :]).astype(BF)
    stepped = jnp.stack([lane(logdec), lane(jax.nn.sigmoid(step_raw + step_bias[None]))])
    px, pd, head, par, gt, last, share_out = back(
        proj, INNER, tail, tb, *prepared, dy, incoming, gcar, one, flag, stepped, inner_t, cotangent[0], remote
    )
    grad_dlog, grad_sbias = head[0, :HEADS], head[1, :HEADS]
    grad_skip = jnp.sum(par[5, :INNER].reshape(HEADS, HEAD_DIM), axis=-1)
    grad_taps, grad_cbias = par[:CONV], par[4]
    heads = jnp.concatenate([grad_dlog, grad_skip, grad_sbias])
    count_in = weight_in.shape[1]
    if own:
        smalls = [
            grad_gated.reshape(devices, -1),
            grad_taps.reshape(CONV, devices, -1).transpose(1, 0, 2).reshape(devices, -1),
            grad_cbias.reshape(devices, -1),
            jnp.broadcast_to(heads[None], (devices, heads.shape[0])),
        ]
        smalls = jnp.concatenate(smalls, axis=1)
        smalls = jnp.pad(smalls, ((0, 0), (0, 1024 - smalls.shape[1]))).reshape(nz, 2, 2, 2, 8, 128)
        gain_row = jnp.broadcast_to(pre_gain[None], (8, width))
        share_in, share, input_grad = scatter(
            normed_t, cotangent[0], dz, px, pd, full, hidden[0], gain_row, smalls, gt, last, nz
        )
        share_in = share_in[:, :count_in]
        flat = share.reshape(-1)
        cuts = [0]
        for s in sizes[1:] + (heads.shape[0],):
            cuts.append(cuts[-1] + s)
        own_gated, own_taps, own_cbias, heads = [flat[a:b] for a, b in zip(cuts, cuts[1:])]
        own_pre, own_taps = share[7, : sizes[0]], own_taps.reshape(CONV, -1)
    else:
        returned = passed_along(gt[8 - CONV + 1 :].astype(BF), "seq", -1).astype(F32)
        px = px.at[piece - CONV + 1 :].set((last[8 - CONV + 1 :] + returned).astype(BF))
        proj_grad = jnp.concatenate([dz, px, pd], axis=1)
        grad_wout = jnp.dot(inner_t, cotangent[0], preferred_element_type=F32)
        grad_win = jnp.dot(normed.T, proj_grad[:, :count_in], preferred_element_type=F32)
        normed_grad = jnp.dot(proj_grad, w_in.T, preferred_element_type=F32)
        unit = rows * scale
        grad_pre = jnp.sum(normed_grad * unit, axis=0)
        pulled = normed_grad * pre_gain
        pulled = scale * (pulled - unit * jnp.mean(pulled * unit, axis=-1, keepdims=True))
        input_grad = cotangent[0].astype(F32) + pulled

        def scattered(total):
            return lax.psum_scatter(total.astype(BF), BOTH, scatter_dimension=0, tiled=True).astype(F32)

        share_in, share_out = scattered(grad_win), scattered(grad_wout)
        smalls = (grad_pre, grad_gated, grad_taps.reshape(-1), grad_cbias, heads)
        summed = lax.psum(jnp.concatenate(smalls), BOTH)
        pieces, start = [], 0
        for s in smalls:
            pieces.append(summed[start : start + s.shape[0]])
            start += s.shape[0]
        own_pre, own_gated = [lax.dynamic_slice_in_dim(pieces[n], me * sizes[n], sizes[n]) for n in range(2)]
        own_taps = lax.dynamic_slice_in_dim(
            pieces[2].reshape(CONV, XBC), me * conv_taps.shape[1], conv_taps.shape[1], axis=1
        )
        own_cbias = lax.dynamic_slice_in_dim(pieces[3], me * sizes[3], sizes[3])
        heads = pieces[4]
    sum_dlog, sum_skip, sum_sbias = [heads[n * HEADS : (n + 1) * HEADS] for n in range(3)]
    grads = (share_in, share_out, own_pre, own_gated, own_taps, own_cbias, sum_dlog, sum_skip, sum_sbias)
    weights = (
        weight_in,
        weight_out,
        gain_pre,
        gain_gated,
        conv_taps,
        conv_bias,
        decay_log,
        skip_gain,
        step_bias,
    )
    means = (
        mean_weight_in,
        mean_weight_out,
        mean_gain_pre,
        mean_gain_gated,
        mean_conv_taps,
        mean_conv_bias,
        mean_decay_log,
        mean_skip_gain,
        mean_step_bias,
    )
    squares = (
        square_weight_in,
        square_weight_out,
        square_gain_pre,
        square_gain_gated,
        square_conv_taps,
        square_conv_bias,
        square_decay_log,
        square_skip_gain,
        square_step_bias,
    )
    rates = (0.01, 0.01, 0.1, 0.1, 0.1, 0.1, 0.1, 0.1, 0.1)
    decays = (0.1, 0.1, 0.0, 0.0, 0.0, 0.0, 0.0, 0.0, 0.0)
    updated = [
        adamw(weights[index], grads[index], means[index], squares[index], rates[index], decays[index])
        for index in range(9)
    ]
    new_weights = tuple((entry[0] for entry in updated))
    new_means = tuple((entry[1] for entry in updated))
    new_squares = tuple((entry[2] for entry in updated))
    return (output[None], input_grad[None]) + grads + new_weights + new_means + new_squares


def solution(mesh):
    dp, seq, both = P("dp"), P("seq"), P(BOTH)
    rows, cols, copied = P(BOTH, None), P(None, BOTH), P()
    whole = P("dp", "seq", None)
    kinds = (rows, rows, both, both, cols, both, copied, copied, copied)
    pairs = tuple(kind for kind in kinds for _ in range(2))
    return jax.shard_map(
        shards,
        mesh=mesh,
        in_specs=(whole, whole, P("dp", None)) + kinds + pairs,
        out_specs=(whole, whole) + kinds * 4,
        check_vma=False,
    )
```
